128 devices in a mesh: rep: 4 (over y_hi, core), dp: 32 (over y_lo, z, x).
Axes of the slice: x: 4, y: 4 (y_hi: 2, y_lo: 2; y = y_hi * 2 + y_lo), z: 4, core: 2. Of those that a mesh axis runs over, the one named last changes fastest.
Arguments:
- query_states: bfloat16 [1024, 32, 768], P(('rep', 'dp')), may hold values from -12 to 12
- passage_states: bfloat16 [512, 180, 768], P(('rep', 'dp')), may hold values from -12 to 12
- query_lengths: int32 [1024], P(('rep', 'dp')), may hold values from 8 to 32, as said below
- passage_lengths: int32 [512], P(('rep', 'dp')), may hold values from 45 to 180, as said below
- passage_ids: int32 [512, 180], P(('rep', 'dp')), may hold values from 2 to 30521, as said below
- positives: int32 [1024], P(('rep', 'dp')), may hold values from 0 to 127, as said below
- up_weight: bfloat16 [768, 3072], replicated, may hold values from -0.21875 to 0.21875
- up_bias: float32 [3072], replicated, may hold values from -3 to 3
- down_weight: bfloat16 [3072, 768], replicated, may hold values from -0.109375 to 0.109375
- down_bias: float32 [768], replicated, may hold values from -3 to 3
- norm_gain: float32 [768], replicated, may hold values from 0.5 to 1.5
- norm_bias: float32 [768], replicated, may hold values from -2 to 2
- proj_weight: bfloat16 [768, 128], replicated, may hold values from -0.21875 to 0.21875
Outputs:
- mean_loss: float32 [], replicated
- passage_grad: float32 [512, 180, 128], P(('rep', 'dp'))
- proj_grad: float32 [768, 128], replicated
The draws below stay inside these ranges and needn't reach their ends.
Inputs may be any that keep to these rules, and one draw needn't show every extreme that they name: `query_lengths`: every device holds a query with all 32 slots real. `passage_lengths`: every device holds a passage with all 180 slots real. `passage_ids`: slots 0 and 1 of every passage hold ids 101 and 2; ids 999 to 1066 are punctuation. `positives`: index of the positive passage among the 128 passages of the query's replica group, in the order of the devices.
All inputs are finite; a program needn't handle non-finite values.
Results may differ from the reference program's by a relative error of at most 0.0055.
Values may be sent and summed in bfloat16 or wider, within the bound.
No kernel may reach another device: no remote copies, remote signals or barrier semaphores. Data moves between devices by JAX's collectives and lax.ppermute only.
A program may use at most 128 MiB of HBM per device.

```python
import jax
import jax.numpy as jnp
from jax import lax

D = 768
FF = 3072
EMB = 128
QLEN = 32
PLEN = 180
Q_DEV = 8
P_DEV = 4
GROUP_Q = 256
GROUP_P = 128
QUERIES = 1024
PASSAGES = 512
N_REP = 4
N_DP = 32


vocab_top = 30522


punct_low = 999


punct_high = 1067


def integer_tables(key):
    folded = jax.random.fold_in(key, 4711)
    subkeys = jax.random.split(folded, 9)
    pass_lengths = jax.random.randint(subkeys[0], (PASSAGES,), PLEN // 4, PLEN + 1)
    pass_full = jax.random.randint(subkeys[1], (PASSAGES // P_DEV,), 0, P_DEV)
    pass_mark = (jnp.arange(P_DEV)[None, :] == pass_full[:, None]).reshape(PASSAGES)
    pass_lengths = jnp.where(pass_mark, PLEN, pass_lengths).astype(jnp.int32)
    query_lengths = jax.random.randint(subkeys[2], (QUERIES,), QLEN // 4, QLEN + 1)
    query_full = jax.random.randint(subkeys[3], (QUERIES // Q_DEV,), 0, Q_DEV)
    query_mark = (jnp.arange(Q_DEV)[None, :] == query_full[:, None]).reshape(QUERIES)
    query_lengths = jnp.where(query_mark, QLEN, query_lengths).astype(jnp.int32)
    is_punct = jax.random.randint(subkeys[4], (PASSAGES, PLEN), 0, 100) < 15
    punct_ids = jax.random.randint(subkeys[5], (PASSAGES, PLEN), punct_low, punct_high)
    word_ids = jax.random.randint(subkeys[6], (PASSAGES, PLEN), 1999, vocab_top)
    token_ids = jnp.where(is_punct, punct_ids, word_ids)
    column = jnp.arange(PLEN)[None, :]
    token_ids = jnp.where(column == 0, 101, jnp.where(column == 1, 2, token_ids)).astype(jnp.int32)
    positives = jax.random.randint(subkeys[7], (QUERIES,), 0, GROUP_P).astype(jnp.int32)
    return (query_lengths, pass_lengths, token_ids, positives)


def passage_tables(key):
    folded = jax.random.fold_in(key, 5813)
    subkeys = jax.random.split(folded, 3)
    states = jax.random.normal(subkeys[0], (PASSAGES, PLEN, D), jnp.float32)
    return jnp.clip(states, -12.0, 12.0)


def draw_passage_states(key, part):
    return passage_tables(key).astype(jnp.bfloat16)


def draw_query_states(key, part):
    query_lengths, pass_lengths, token_ids, positives = integer_tables(key)
    states = passage_tables(key)
    folded = jax.random.fold_in(key, 6907)
    subkeys = jax.random.split(folded, 4)
    group_index = jnp.arange(QUERIES) // GROUP_Q
    target = group_index * GROUP_P + positives
    pick_pos = jax.random.randint(subkeys[0], (QUERIES, QLEN), 0, 1 << 20) % pass_lengths[target][:, None]
    copied = states[target[:, None], pick_pos]
    noise_part = jax.random.normal(subkeys[1], (QUERIES, QLEN, D), jnp.float32)
    copy_flag = jax.random.randint(subkeys[2], (QUERIES, QLEN), 0, 2) == 1
    blended = jnp.where(copy_flag[:, :, None], 0.7 * copied + 0.7 * noise_part, noise_part)
    return jnp.clip(blended, -12.0, 12.0).astype(jnp.bfloat16)


def draw_query_lengths(key, part):
    return integer_tables(key)[0]


def draw_passage_lengths(key, part):
    return integer_tables(key)[1]


def draw_passage_ids(key, part):
    return integer_tables(key)[2]


def draw_positives(key, part):
    return integer_tables(key)[3]


def scatter_about(rng, extent, deviation, limit, held_as=jnp.bfloat16):
    values = deviation * jax.random.normal(rng, extent, jnp.float32)
    return jnp.clip(values, min=-limit, max=limit).astype(held_as)


def setup_inputs(seed: int = 0) -> dict:
    keys = jax.random.split(jax.random.key(seed), 14)
    query_states = draw_query_states(jax.random.fold_in(keys[13], 71), 0)
    passage_states = draw_passage_states(jax.random.fold_in(keys[13], 71), 0)
    query_lengths = draw_query_lengths(jax.random.fold_in(keys[13], 71), 0)
    passage_lengths = draw_passage_lengths(jax.random.fold_in(keys[13], 71), 0)
    passage_ids = draw_passage_ids(jax.random.fold_in(keys[13], 71), 0)
    positives = draw_positives(jax.random.fold_in(keys[13], 71), 0)
    up_weight = scatter_about(keys[6], (D, FF), D ** -0.5, 0.21875)
    up_bias = scatter_about(keys[7], (FF,), 0.5, 3.0, jnp.float32)
    down_weight = scatter_about(keys[8], (FF, D), FF ** -0.5, 0.109375)
    down_bias = scatter_about(keys[9], (D,), 0.5, 3.0, jnp.float32)
    norm_gain = jnp.clip(1.0 + 0.1 * jax.random.normal(keys[10], (D,), jnp.float32), 0.5, 1.5)
    norm_bias = scatter_about(keys[11], (D,), 0.3, 2.0, jnp.float32)
    proj_weight = scatter_about(keys[12], (D, EMB), D ** -0.5, 0.21875)
    return {"query_states": query_states, "passage_states": passage_states, "query_lengths": query_lengths, "passage_lengths": passage_lengths, "passage_ids": passage_ids, "positives": positives, "up_weight": up_weight, "up_bias": up_bias, "down_weight": down_weight, "down_bias": down_bias, "norm_gain": norm_gain, "norm_bias": norm_bias, "proj_weight": proj_weight}


temper = 0.05
eps_norm = 1e-06
punct_low = 999
punct_high = 1067

def encode_rows(token_rows, up_weight, up_bias, down_weight, down_bias, norm_gain, norm_bias, proj_weight):
    upward = jnp.dot(token_rows, up_weight, preferred_element_type=jnp.float32) + up_bias
    activated = jax.nn.gelu(upward, approximate=False).astype(jnp.bfloat16)
    residual = token_rows.astype(jnp.float32) + jnp.dot(activated, down_weight, preferred_element_type=jnp.float32) + down_bias
    average = lax.optimization_barrier(jnp.mean(residual, -1, keepdims=True))
    centered = residual - average
    variance = lax.optimization_barrier(jnp.mean(centered * centered, -1, keepdims=True))
    hidden = (centered * lax.rsqrt(variance + eps_norm) * norm_gain + norm_bias).astype(jnp.bfloat16)
    projected = jnp.dot(hidden, proj_weight, preferred_element_type=jnp.float32)
    inverse = lax.rsqrt(lax.optimization_barrier(jnp.sum(projected * projected, -1, keepdims=True)) + eps_norm)
    return (hidden, projected * inverse, inverse)

def token_scores(query_flat, query_keep, block_emb, block_keep, query_count):
    item_count, pass_len, embed_dim = block_emb.shape
    similar = jnp.dot(query_flat, block_emb.reshape(item_count * pass_len, embed_dim).T, preferred_element_type=jnp.float32)
    weights = jnp.exp(similar / temper).reshape(-1, item_count, pass_len) * block_keep.astype(jnp.float32)[None]
    totals = lax.optimization_barrier(jnp.sum(weights, -1))
    soft_max = temper * jnp.log(totals) * query_keep[:, None]
    scores = lax.optimization_barrier(jnp.sum(soft_max.reshape(query_count, -1, item_count), 1))
    return (scores, weights, totals)

def token_grads(query_flat, query_keep, block_emb, weights, totals, dscore, query_count):
    item_count, pass_len, embed_dim = block_emb.shape
    factor = (dscore[:, None, :] * query_keep.reshape(query_count, -1)[:, :, None]).reshape(-1, item_count) / totals
    sim_grad = (weights * factor[:, :, None]).reshape(-1, item_count * pass_len).astype(jnp.bfloat16)
    passage_term = jnp.dot(sim_grad.T, query_flat, preferred_element_type=jnp.float32)
    query_term = jnp.dot(sim_grad, block_emb.reshape(item_count * pass_len, embed_dim), preferred_element_type=jnp.float32)
    return (passage_term.reshape(item_count, pass_len, embed_dim), query_term)

def cross_entropy(scores, positives):
    log_total = jnp.log(lax.optimization_barrier(jnp.sum(jnp.exp(scores), 1)))
    onehot = (jnp.arange(scores.shape[1], dtype=jnp.int32)[None, :] == positives[:, None]).astype(jnp.float32)
    loss_sum = jnp.sum(log_total - lax.optimization_barrier(jnp.sum(scores * onehot, 1)))
    dscore = jnp.exp(scores - log_total[:, None]) - onehot
    return (loss_sum, dscore)

def norm_backward(gradient, normed, inverse):
    return (inverse * (gradient - normed * lax.optimization_barrier(jnp.sum(normed * gradient, -1, keepdims=True)))).astype(jnp.bfloat16)

def reference(query_states, passage_states, query_lengths, passage_lengths, passage_ids, positives, up_weight, up_bias, down_weight, down_bias, norm_gain, norm_bias, proj_weight):

    def encode_all(states, per_block):
        item_count, length, model_width = states.shape
        blocks = states.reshape(item_count // per_block, per_block * length, model_width)

        def encode_block(block):
            return encode_rows(block, up_weight, up_bias, down_weight, down_bias, norm_gain, norm_bias, proj_weight)
        hidden, normed, inverse = lax.map(encode_block, blocks)
        return (hidden.reshape(-1, model_width), normed.reshape(-1, EMB), inverse.reshape(-1, 1))
    query_hidden, query_normed, query_inverse = encode_all(query_states, Q_DEV)
    pass_hidden, pass_normed, pass_inverse = encode_all(passage_states, P_DEV)
    query_emb = query_normed.astype(jnp.bfloat16).reshape(N_REP, N_DP, Q_DEV * QLEN, EMB)
    query_keep = (jnp.arange(QLEN, dtype=jnp.int32)[None, :] < query_lengths[:, None]).astype(jnp.float32)
    query_keep = query_keep.reshape(N_REP, N_DP, Q_DEV * QLEN)
    is_punct = (passage_ids >= punct_low) & (passage_ids < punct_high)
    pass_keep = ((jnp.arange(PLEN, dtype=jnp.int32)[None, :] < passage_lengths[:, None]) & jnp.logical_not(is_punct)).astype(jnp.float32)
    pass_keep = pass_keep.reshape(N_REP, GROUP_P, PLEN)
    pass_emb = pass_normed.astype(jnp.bfloat16).reshape(N_REP, GROUP_P, PLEN, EMB)
    grouped_pos = positives.reshape(N_REP, N_DP, Q_DEV)

    def one_group(operands):
        group_query, group_qkeep, group_pass, group_pkeep, group_pos = operands

        def advance(pass_grad, block):
            block_query, block_keep, block_pos = block
            scores, weights, totals = token_scores(block_query, block_keep, group_pass, group_pkeep, Q_DEV)
            loss_sum, dscore = cross_entropy(scores, block_pos)
            passage_term, query_term = token_grads(block_query, block_keep, group_pass, weights, totals, dscore, Q_DEV)
            return (pass_grad + passage_term, (loss_sum, query_term))
        start_grad = jnp.zeros((GROUP_P, PLEN, EMB), jnp.float32)
        pass_grad, (losses, query_terms) = lax.scan(advance, start_grad, (group_query, group_qkeep, group_pos))
        return (pass_grad, jnp.sum(losses), query_terms)
    pass_grad, losses, query_grad = lax.map(one_group, (query_emb, query_keep, pass_emb, pass_keep, grouped_pos))
    passage_grad = pass_grad.reshape(PASSAGES, PLEN, EMB)
    mean_loss = jnp.sum(losses) / QUERIES
    query_back = norm_backward(query_grad.reshape(-1, EMB), query_normed, query_inverse)
    pass_back = norm_backward(passage_grad.reshape(-1, EMB), pass_normed, pass_inverse)
    proj_grad = jnp.dot(query_hidden.T, query_back, preferred_element_type=jnp.float32) + jnp.dot(pass_hidden.T, pass_back, preferred_element_type=jnp.float32)
    return (mean_loss, passage_grad, proj_grad)
```

```python
import functools

import jax
import jax.numpy as jnp
from jax import lax
from jax.experimental import pallas as pl
from jax.experimental.pallas import tpu as pltpu
from jax.sharding import PartitionSpec as P

temper = 0.05
eps_norm = 1e-06
punct_low = 999
punct_high = 1067

bf16 = jnp.bfloat16
f32 = jnp.float32


X_PEERS = 4
YZ_PEERS = 8
PAD = 192
FCHUNK = 512
MASKED = 2.0
BIAS = -10000.0
SCALE = 1.4426950408889634 / temper


def mm(a, b):
    return jnp.dot(a, b, preferred_element_type=f32)


def encode_kernel(
    qlen_ref, pos_ref, plen_ref, ids_ref, xq_ref, xp_ref, w1_ref, b1_ref, w2_ref, b2_ref,
    gain_ref, nbias_ref, proj_ref, hidden_ref, projected_ref, qsend_ref, psend_ref,
    x_s, acc_s, keep_s, ids_s,
):
    step = pl.program_id(0)
    q_dev, q_len, width = xq_ref.shape
    p_dev, p_len, _ = xp_ref.shape
    q_rows = q_dev * q_len
    rows = x_s.shape[0]
    tile = 256

    @pl.when(step == 0)
    def _():
        for q in range(q_dev):
            x_s[q * q_len : (q + 1) * q_len, :] = xq_ref[q]
        for p in range(p_dev):
            base = q_rows + p * PAD
            x_s[base + PAD - 16 : base + PAD, :] = jnp.zeros((16, width), bf16)
            x_s[base : base + p_len, :] = xp_ref[p]
        ids_s[...] = jnp.zeros_like(ids_s)
        ids_s[0:p_dev, 0:p_len] = ids_ref[...]
        row_i = lax.broadcasted_iota(jnp.int32, (PAD, 256), 0)
        col_i = lax.broadcasted_iota(jnp.int32, (PAD, 256), 1)
        col_1 = lax.broadcasted_iota(jnp.int32, (1, 256), 1)
        ones = jnp.ones((256, 128), bf16)
        for p in range(p_dev):
            ids = ids_s[p : p + 1, :]
            punct = jnp.logical_and(ids >= punct_low, ids < punct_high)
            keep = jnp.logical_and(col_1 < plen_ref[p], jnp.logical_not(punct))
            keep = jnp.where(keep, 1.0, 0.0)
            diag = jnp.where(row_i == col_i, keep, 0.0).astype(bf16)
            keep_s[p * PAD : (p + 1) * PAD, :] = mm(diag, ones)

    def ffn(m):
        r = slice(m * tile, (m + 1) * tile)
        up = mm(x_s[r, :], w1_ref[...]) + b1_ref[...]
        half = up * 0.5
        act = (half + half * lax.erf(up * 0.7071067811865476)).astype(bf16)
        return r, mm(act, w2_ref[...])

    @pl.when(step == 0)
    def _():
        for m in range(rows // tile):
            r, part = ffn(m)
            acc_s[r, :] = part

    @pl.when(step > 0)
    def _():
        for m in range(rows // tile):
            r, part = ffn(m)
            acc_s[r, :] += part

    @pl.when(step == pl.num_programs(0) - 1)
    def _():
        for m in range(rows // tile):
            r = slice(m * tile, (m + 1) * tile)
            res = x_s[r, :].astype(f32) + acc_s[r, :] + b2_ref[...]
            mean = jnp.sum(res, -1, keepdims=True) * (1.0 / width)
            cen = res - mean
            var = jnp.sum(cen * cen, -1, keepdims=True) * (1.0 / width)
            hid = (cen * lax.rsqrt(var + eps_norm) * gain_ref[...] + nbias_ref[...]).astype(bf16)
            hidden_ref[r, :] = hid
            pr = mm(hid, proj_ref[...])
            projected_ref[r, :] = pr
            inv = lax.rsqrt(jnp.sum(pr * pr, -1, keepdims=True) + eps_norm)
            normed = pr * inv
            if m * tile < q_rows:
                qsend_ref[r, :] = normed.astype(bf16)
            else:
                s = slice(m * tile - q_rows, (m + 1) * tile - q_rows)
                psend_ref[s, :] = jnp.where(keep_s[s, :] > 0.5, normed, MASKED).astype(bf16)
        row = lax.broadcasted_iota(jnp.int32, (16, 128), 0)
        token = lax.broadcasted_iota(jnp.int32, (16, 128), 1) + 128 * (row % 2)
        owner = token // q_len
        slot = token % q_len
        lens = jnp.zeros((16, 128), jnp.int32)
        posi = jnp.zeros((16, 128), jnp.int32)
        for q in range(q_dev):
            lens = jnp.where(owner == q, qlen_ref[q], lens)
            posi = jnp.where(owner == q, pos_ref[q], posi)
        kept = jnp.where(slot < lens, 1.0, 0.0)
        meta = jnp.where(row < 2, kept, jnp.where(row < 4, posi.astype(f32), 0.0))
        qsend_ref[q_rows : q_rows + 16, :] = meta.astype(bf16)


def encode(xq, xp, qlen, plen, ids, pos, w1, b1, w2, b2, gain, nbias, proj):
    width, ff = w1.shape
    emb = proj.shape[1]
    q_rows = xq.shape[0] * xq.shape[1]
    p_rows = xp.shape[0] * PAD
    rows = q_rows + p_rows
    smem = pl.BlockSpec(memory_space=pltpu.SMEM)

    def whole(*shape):
        return pl.BlockSpec(shape, lambda k: (0,) * len(shape))

    return pl.pallas_call(
        encode_kernel,
        grid=(ff // FCHUNK,),
        in_specs=[
            smem, smem, smem, whole(*ids.shape), whole(*xq.shape), whole(*xp.shape),
            pl.BlockSpec((width, FCHUNK), lambda k: (0, k)),
            pl.BlockSpec((1, FCHUNK), lambda k: (0, k)),
            pl.BlockSpec((FCHUNK, width), lambda k: (k, 0)),
            whole(1, width), whole(1, width), whole(1, width), whole(width, emb),
        ],
        out_specs=[whole(rows, width), whole(rows, emb), whole(q_rows + 16, emb), whole(p_rows, emb)],
        out_shape=[
            jax.ShapeDtypeStruct((rows, width), bf16),
            jax.ShapeDtypeStruct((rows, emb), f32),
            jax.ShapeDtypeStruct((q_rows + 16, emb), bf16),
            jax.ShapeDtypeStruct((p_rows, emb), bf16),
        ],
        scratch_shapes=[
            pltpu.VMEM((rows, width), bf16),
            pltpu.VMEM((rows, width), f32),
            pltpu.VMEM((p_rows, emb), f32),
            pltpu.VMEM((8, 256), jnp.int32),
        ],
        compiler_params=pltpu.CompilerParams(dimension_semantics=("arbitrary",)),
        name="encode",
    )(qlen, pos, plen, ids, xq, xp, w1, b1[None], w2, b2[None], gain[None], nbias[None], proj)


def load_pairs(q_refs, p_refs, qt_s, pa_s, keep_s):
    emb = 128
    for k, q_ref in enumerate(q_refs):
        qt_s[0:emb, k * 256 : (k + 1) * 256] = q_ref[0:256, :].T
        for h in range(2):
            keep_s[:, k * 256 + h * 128 : k * 256 + (h + 1) * 128] = q_ref[256 + h : 257 + h, :].astype(f32)
    cols = qt_s.shape[1]
    first = lax.broadcasted_iota(jnp.int32, (emb, cols), 0) == 0
    qt_s[emb : 2 * emb, :] = jnp.where(first, 1.0, 0.0).astype(bf16)
    for k, p_ref in enumerate(p_refs):
        r = slice(k * 4 * PAD, (k + 1) * 4 * PAD)
        val = p_ref[...]
        pa_s[r, 0:emb] = val
        pa_s[r, emb : 2 * emb] = jnp.where(val.astype(f32) > 1.5, BIAS, 0.0).astype(bf16)


def forward_kernel(yz_ref, *refs):
    q_refs, p_refs = refs[:YZ_PEERS], refs[YZ_PEERS : YZ_PEERS + X_PEERS]
    sc_ref, tot_ref, zsend_ref, qt_s, pa_s, keep_s = refs[YZ_PEERS + X_PEERS :]
    load_pairs(q_refs, p_refs, qt_s, pa_s, keep_s)
    cols = qt_s.shape[1]

    def group(g, carry):
        for i in range(4):
            p = g * 4 + i
            lhs = pa_s[pl.ds(pl.multiple_of(p * PAD, PAD), PAD), :]
            for j in range(cols // 256):
                c = slice(j * 256, (j + 1) * 256)
                e = jnp.exp2(mm(lhs, qt_s[:, c]) * SCALE)
                tot_ref[pl.ds(p, 1), c] = jnp.sum(e, axis=0, keepdims=True)
        return carry

    lax.fori_loop(0, 4, group, 0)
    a = lax.broadcasted_iota(jnp.int32, (128, 128), 0) // 32
    b = lax.broadcasted_iota(jnp.int32, (128, 128), 1) // 32
    same = jnp.where(a == b, 1.0, 0.0)
    for t in range(cols // 128):
        c = slice(t * 128, (t + 1) * 128)
        soft = jnp.log(tot_ref[:, c]) * temper * keep_s[:, c]
        sc = jnp.dot(soft, same, preferred_element_type=f32, precision=lax.Precision.HIGHEST)
        sc_ref[:, c] = sc
        z = jnp.sum(jnp.exp(sc), axis=0, keepdims=True)
        row = yz_ref[t // 2] * 2 + t % 2
        for k in range(YZ_PEERS):
            zsend_ref[k, pl.ds(row, 1), :] = z


def forward(yz, qs, ps):
    cols = YZ_PEERS * 256
    vm = pl.BlockSpec(memory_space=pltpu.VMEM)
    smem = pl.BlockSpec(memory_space=pltpu.SMEM)
    return pl.pallas_call(
        forward_kernel,
        in_specs=[smem] + [vm] * (YZ_PEERS + X_PEERS),
        out_specs=[vm] * 3,
        out_shape=[
            jax.ShapeDtypeStruct((16, cols), f32),
            jax.ShapeDtypeStruct((16, cols), f32),
            jax.ShapeDtypeStruct((YZ_PEERS, 16, 128), f32),
        ],
        scratch_shapes=[
            pltpu.VMEM((256, cols), bf16),
            pltpu.VMEM((16 * PAD, 256), bf16),
            pltpu.VMEM((1, cols), f32),
        ],
        name="pair_forward",
    )(yz, *qs, *ps)


def backward_kernel(yz_ref, pid_ref, *refs):
    q_refs, p_refs = refs[:YZ_PEERS], refs[YZ_PEERS : YZ_PEERS + X_PEERS]
    refs = refs[YZ_PEERS + X_PEERS :]
    sc_ref, tot_ref, z_ref = refs[:3]
    dp_refs, dq_refs, loss_ref = refs[3 : 3 + X_PEERS], refs[3 + X_PEERS : 3 + X_PEERS + YZ_PEERS], refs[3 + X_PEERS + YZ_PEERS]
    qt_s, pa_s, keep_s, pt_s, q_s, fac_s, g_s, dp_s, dq_s = refs[4 + X_PEERS + YZ_PEERS :]
    load_pairs(q_refs, p_refs, qt_s, pa_s, keep_s)
    cols = qt_s.shape[1]
    for k, p_ref in enumerate(p_refs):
        for i in range(3):
            r = slice(k * 768 + i * 256, k * 768 + (i + 1) * 256)
            pt_s[:, r] = p_ref[i * 256 : (i + 1) * 256, :].T
    for k, q_ref in enumerate(q_refs):
        q_s[k * 256 : (k + 1) * 256, :] = q_ref[0:256, :]
    row = lax.broadcasted_iota(jnp.int32, (16, 128), 0)
    number = jnp.zeros((16, 128), jnp.int32)
    for k in range(X_PEERS):
        number = jnp.where(row // 4 == k, pid_ref[k] + row % 4, number)
    number = number.astype(f32)
    lane = lax.broadcasted_iota(jnp.int32, (1, 128), 1)
    head = jnp.where(lane % 32 == 0, 1.0, 0.0)
    loss = jnp.zeros((1, 128), f32)
    for t in range(cols // 128):
        c = slice(t * 128, (t + 1) * 128)
        zrow = yz_ref[t // 2] * 2 + t % 2
        z = z_ref[0, pl.ds(zrow, 1), :]
        for k in range(1, YZ_PEERS):
            z = z + z_ref[k, pl.ds(zrow, 1), :]
        sc = sc_ref[:, c]
        pos = q_refs[t // 2][258 + t % 2 : 259 + t % 2, :].astype(f32)
        hit = jnp.where(number == pos, 1.0, 0.0)
        fac_s[:, c] = (jnp.exp(sc) / z - hit) * (keep_s[:, c] / tot_ref[:, c])
        loss = loss - jnp.sum(hit * sc, axis=0, keepdims=True) * head
        if t < 2:
            loss = loss + jnp.log(z) * head
    loss_ref[...] = jnp.broadcast_to(jnp.sum(loss, axis=1, keepdims=True), loss_ref.shape)

    wide = g_s.shape[1]

    def columns(j, carry):
        base = pl.multiple_of(j * wide, wide)

        def group(g, carry):
            for i in range(4):
                p = g * 4 + i
                r = pl.ds(pl.multiple_of(p * PAD, PAD), PAD)
                lhs = pa_s[r, :]
                for h in range(wide // 256):
                    c = pl.ds(base + h * 256, 256)
                    e = jnp.exp2(mm(lhs, qt_s[:, c]) * SCALE)
                    g_s[r, h * 256 : (h + 1) * 256] = (e * fac_s[pl.ds(p, 1), c]).astype(bf16)
            return carry

        lax.fori_loop(0, 4, group, 0)
        dq_s[:, pl.ds(base, wide)] = mm(pt_s[...], g_s[...]).astype(bf16)
        qb = q_s[pl.ds(base, wide), :]

        def rows(m, carry):
            r = pl.ds(pl.multiple_of(m * 768, 768), 768)
            part = mm(g_s[r, :], qb)
            dp_s[r, :] = jnp.where(j == 0, part, dp_s[r, :] + part)
            return carry

        lax.fori_loop(0, 4, rows, 0)
        return carry

    lax.fori_loop(0, cols // wide, columns, 0)
    for k in range(X_PEERS):
        dp_refs[k][...] = dp_s[k * 768 : (k + 1) * 768, :].astype(bf16)
    for k in range(YZ_PEERS):
        dq_refs[k][...] = dq_s[:, k * 256 : (k + 1) * 256]


def backward(yz, pid, qs, ps, sc, tot, z):
    cols = YZ_PEERS * 256
    vm = pl.BlockSpec(memory_space=pltpu.VMEM)
    smem = pl.BlockSpec(memory_space=pltpu.SMEM)
    wide = 512
    out = pl.pallas_call(
        backward_kernel,
        in_specs=[smem, smem] + [vm] * (YZ_PEERS + X_PEERS + 3),
        out_specs=[vm] * (X_PEERS + YZ_PEERS + 1),
        out_shape=[jax.ShapeDtypeStruct((4 * PAD, 128), bf16)] * X_PEERS
        + [jax.ShapeDtypeStruct((128, 256), bf16)] * YZ_PEERS
        + [jax.ShapeDtypeStruct((1, 128), f32)],
        scratch_shapes=[
            pltpu.VMEM((256, cols), bf16),
            pltpu.VMEM((16 * PAD, 256), bf16),
            pltpu.VMEM((1, cols), f32),
            pltpu.VMEM((128, 16 * PAD), bf16),
            pltpu.VMEM((cols, 128), bf16),
            pltpu.VMEM((16, cols), f32),
            pltpu.VMEM((16 * PAD, wide), bf16),
            pltpu.VMEM((16 * PAD, 128), f32),
            pltpu.VMEM((128, cols), bf16),
        ],
        name="pair_backward",
    )(yz, pid, *qs, *ps, sc, tot, z)
    return out[:X_PEERS], out[X_PEERS : X_PEERS + YZ_PEERS], out[-1]


def final_kernel(*refs):
    dp_refs, dq_refs = refs[:X_PEERS], refs[X_PEERS : X_PEERS + YZ_PEERS]
    projected_ref, hidden_ref, loss_ref, pgrad_ref, share_ref, bt_s = refs[X_PEERS + YZ_PEERS :]
    p_dev, p_len, _ = pgrad_ref.shape
    pr = projected_ref[0:256, :]
    inv = lax.rsqrt(jnp.sum(pr * pr, -1, keepdims=True) + eps_norm)
    nt = (pr * inv).T
    it = jnp.broadcast_to(inv, pr.shape).T
    grad = dq_refs[0][...].astype(f32)
    for k in range(1, YZ_PEERS):
        grad = grad + dq_refs[k][...].astype(f32)
    dot = jnp.sum(nt * grad, axis=0, keepdims=True)
    bt_s[:, 0:256] = (it * (grad - nt * dot)).astype(bf16)
    for p in range(p_dev):
        r = slice(p * PAD, (p + 1) * PAD)
        grad = dp_refs[0][r, :].astype(f32)
        for k in range(1, X_PEERS):
            grad = grad + dp_refs[k][r, :].astype(f32)
        pgrad_ref[p] = grad[:p_len, :]
        pr = projected_ref[256 + p * PAD : 256 + (p + 1) * PAD, :]
        inv = lax.rsqrt(jnp.sum(pr * pr, -1, keepdims=True) + eps_norm)
        nm = pr * inv
        back = inv * (grad - nm * jnp.sum(nm * grad, -1, keepdims=True))
        bt_s[:, 256 + p * PAD : 256 + (p + 1) * PAD] = back.T.astype(bf16)
    for k in range(6):
        pg = mm(bt_s[...], hidden_ref[:, k * 128 : (k + 1) * 128])
        share_ref[:, k, :] = pg.T.astype(bf16).astype(f32)
    loss = loss_ref[...]
    high = loss.astype(bf16).astype(f32)
    share_ref[:, 6, :] = jnp.broadcast_to(high, (128, 128))
    share_ref[:, 7, :] = jnp.broadcast_to(loss - high, (128, 128))


def final(dps, dqs, projected, hidden, loss, p_dev, p_len):
    vm = pl.BlockSpec(memory_space=pltpu.VMEM)
    return pl.pallas_call(
        final_kernel,
        in_specs=[vm] * (X_PEERS + YZ_PEERS + 3),
        out_specs=[vm] * 2,
        out_shape=[
            jax.ShapeDtypeStruct((p_dev, p_len, 128), f32),
            jax.ShapeDtypeStruct((128, 8, 128), f32),
        ],
        scratch_shapes=[pltpu.VMEM((128, hidden.shape[0]), bf16)],
        name="final_grad",
    )(*dps, *dqs, projected, hidden, loss)


def x_ring(k):
    return [(j, (j // 4) * 4 + (j % 4 + k) % 4) for j in range(32)]


def yz_step(k):
    def to(j):
        yz, x = j // 4, j % 4
        y, z = yz // 4, yz % 4
        return ((y ^ (k // 4)) * 4 + (z + k % 4) % 4) * 4 + x

    return [(j, to(j)) for j in range(32)]


def inverse(pairs):
    return [(b, a) for a, b in pairs]


def per_device(
    query_states, passage_states, query_lengths, passage_lengths, passage_ids, positives,
    up_weight, up_bias, down_weight, down_bias, norm_gain, norm_bias, proj_weight,
):
    p_dev, p_len, _ = passage_states.shape
    queries = query_states.shape[0] * lax.axis_size("rep") * lax.axis_size("dp")
    me = lax.axis_index("dp")
    x, yz = me % 4, me // 4
    steps = jnp.arange(YZ_PEERS, dtype=jnp.int32)
    yz_from = ((yz // 4) ^ (steps // 4)) * 4 + (yz % 4 - steps % 4) % 4
    x_from = (x - jnp.arange(X_PEERS, dtype=jnp.int32)) % 4
    first_passage = yz * 16 + x_from * 4

    hidden, projected, qsend, psend = encode(
        query_states, passage_states, query_lengths, passage_lengths, passage_ids, positives,
        up_weight, up_bias, down_weight, down_bias, norm_gain, norm_bias, proj_weight,
    )
    ps = [psend] + [lax.ppermute(psend, "dp", x_ring(k)) for k in range(1, X_PEERS)]
    qs = [qsend] + [lax.ppermute(qsend, "dp", yz_step(k)) for k in range(1, YZ_PEERS)]
    sc, tot, zsend = forward(yz_from, qs, ps)
    yz_groups = [[4 * k + i for k in range(YZ_PEERS)] for i in range(X_PEERS)]
    z = lax.all_to_all(zsend, "dp", 0, 0, axis_index_groups=yz_groups, tiled=True)
    dps, dqs, loss = backward(yz_from, first_passage, qs, ps, sc, tot, z)
    dps = [dps[0]] + [lax.ppermute(dps[k], "dp", inverse(x_ring(k))) for k in range(1, X_PEERS)]
    dqs = [dqs[0]] + [lax.ppermute(dqs[k], "dp", inverse(yz_step(k))) for k in range(1, YZ_PEERS)]
    passage_grad, share = final(dps, dqs, projected, hidden, loss, p_dev, p_len)
    parts = lax.all_to_all(share.astype(bf16), ("rep", "dp"), 0, 0, tiled=True)
    summed = jnp.sum(parts.astype(f32), axis=0)
    mean_loss = (summed[6, 0] + summed[7, 0]) / queries
    out = jnp.broadcast_to(summed.astype(bf16)[None], parts.shape)
    pieces = lax.all_to_all(out, ("rep", "dp"), 0, 0, tiled=True)
    proj_grad = jnp.swapaxes(pieces[:, :6, :], 0, 1).reshape(768, 128).astype(f32)
    return (mean_loss, passage_grad, proj_grad)


def solution(mesh):
    rows = P(("rep", "dp"))
    in_specs = (rows,) * 6 + (P(),) * 7
    out_specs = (P(), rows, P())
    return jax.shard_map(
        per_device, mesh=mesh, in_specs=in_specs, out_specs=out_specs, check_vma=False
    )
```

```python
import jax
import jax.numpy as jnp
from jax import lax
from jax.experimental import pallas as pl
from jax.experimental.pallas import tpu as pltpu
from jax.sharding import PartitionSpec as P

temper = 0.05
eps_norm = 1e-06
punct_low = 999
punct_high = 1067

bf16 = jnp.bfloat16
f32 = jnp.float32
i32 = jnp.int32


X_PEERS = 4
YZ_PEERS = 8
P_ROWS = 720
Q_ROWS = 256
EMB = 128
FCHUNK = 512
MASKED = 2.0
BIAS = -10000.0
SCALE = 1.4426950408889634 / temper

VM = pl.BlockSpec(memory_space=pltpu.VMEM)
SM = pl.BlockSpec(memory_space=pltpu.SMEM)


def mm(a, b):
    return jnp.dot(a, b, preferred_element_type=f32)


def fetch(which, k, w1_ref, w2_ref, w1_s, w2_s, sem):
    c = pl.ds(pl.multiple_of(k * FCHUNK, FCHUNK), FCHUNK)
    if which == 0:
        return pltpu.make_async_copy(w1_ref.at[:, c], w1_s.at[k], sem.at[0, k])
    return pltpu.make_async_copy(w2_ref.at[c, :], w2_s.at[k], sem.at[1, k])


def start_fetch(w1_ref, w2_ref, w1_s, w2_s, sem):
    for k in range(w1_s.shape[0]):
        for which in range(2):
            fetch(which, k, w1_ref, w2_ref, w1_s, w2_s, sem).start()


def feed_forward(w1_ref, b1_ref, w2_ref, x_s, acc_s, act_s, w1_s, w2_s, sem, tile):
    rows = x_s.shape[0]
    count = w1_s.shape[0]

    def up(k, slot):
        fetch(0, k, w1_ref, w2_ref, w1_s, w2_s, sem).wait()
        bias = b1_ref[:, pl.ds(pl.multiple_of(k * FCHUNK, FCHUNK), FCHUNK)]
        for m in range(rows // tile):
            r = slice(m * tile, (m + 1) * tile)
            half = mm(x_s[r, :], w1_s[k]) + bias
            act_s[slot, r, :] = (half * 0.5 * (1.0 + lax.erf(half * 0.7071067811865476))).astype(bf16)

    def down(k, slot):
        for m in range(rows // tile):
            r = slice(m * tile, (m + 1) * tile)
            acc_s[r, :] += mm(act_s[slot, r, :], w2_s[k])

    up(0, 0)

    def step(k, carry):
        fetch(1, k, w1_ref, w2_ref, w1_s, w2_s, sem).wait()
        fetch(0, k + 1, w1_ref, w2_ref, w1_s, w2_s, sem).wait()
        now, later = k % 2, (k + 1) % 2
        bias = b1_ref[:, pl.ds(pl.multiple_of((k + 1) * FCHUNK, FCHUNK), FCHUNK)]
        for m in range(rows // tile):
            r = slice(m * tile, (m + 1) * tile)
            half = mm(x_s[r, :], w1_s[k + 1]) + bias
            act_s[later, r, :] = (half * 0.5 * (1.0 + lax.erf(half * 0.7071067811865476))).astype(bf16)
            acc_s[r, :] += mm(act_s[now, r, :], w2_s[k])
        return carry

    lax.fori_loop(0, count - 1, step, 0)
    fetch(1, count - 1, w1_ref, w2_ref, w1_s, w2_s, sem).wait()
    down(count - 1, (count - 1) % 2)


def finish_rows(r, acc_s, gain, nbias, proj_ref, hidden_ref, projected_ref):
    width = acc_s.shape[1]
    res = acc_s[r, :]
    mean = jnp.sum(res, -1, keepdims=True) * (1.0 / width)
    cen = res - mean
    var = jnp.sum(cen * cen, -1, keepdims=True) * (1.0 / width)
    hid = (cen * lax.rsqrt(var + eps_norm) * gain + nbias).astype(bf16)
    hidden_ref[r, :] = hid
    pr = mm(hid, proj_ref[...])
    projected_ref[r, :] = pr
    return pr * lax.rsqrt(jnp.sum(pr * pr, -1, keepdims=True) + eps_norm)


def encode_kernel(
    qlen_ref, pos_ref, plen_ref, ids_ref, xq_ref, xp_ref, w1_ref, b1_ref, w2_ref, b2_ref,
    gain_ref, nbias_ref, proj_ref, hidden_ref, projected_ref, qsend_ref, psend_ref,
    x_s, acc_s, act_s, w1_s, w2_s, sem, keep_s, ids_s,
):
    start_fetch(w1_ref, w2_ref, w1_s, w2_s, sem)
    q_dev, q_len, width = xq_ref.shape
    p_len, p_dev, _ = xp_ref.shape
    b2, gain, nbias = (v[...].reshape(1, width) for v in (b2_ref, gain_ref, nbias_ref))
    x_s[0:Q_ROWS, :] = xq_ref[...].reshape(Q_ROWS, width)
    x_s[Q_ROWS:, :] = xp_ref[...].reshape(P_ROWS, width)
    acc_s[...] = x_s[...].astype(f32) + b2
    ids_s[...] = jnp.zeros_like(ids_s)
    ids_s[0:p_dev, 0:p_len] = ids_ref[...]
    ids_s[p_dev : 2 * p_dev, 0:p_len] = ids_ref[...]
    ids = ids_s[...]
    row = lax.broadcasted_iota(i32, (8, 256), 0) % p_dev
    col = lax.broadcasted_iota(i32, (8, 256), 1)
    lens = jnp.zeros((8, 256), i32)
    for p in range(p_dev):
        lens = jnp.where(row == p, plen_ref[p], lens)
    punct = jnp.logical_and(ids >= punct_low, ids < punct_high)
    keep = jnp.where(jnp.logical_and(col < lens, jnp.logical_not(punct)), 1.0, 0.0)
    ones = jnp.ones((256, EMB), bf16)
    slab = lax.broadcasted_iota(i32, (30, 8, 256), 0) * 2 + lax.broadcasted_iota(i32, (30, 8, 256), 1) // p_dev
    cols = lax.broadcasted_iota(i32, (30, 8, 256), 2)
    for m in range(3):
        pick = jnp.where(slab + m * 60 == cols, jnp.broadcast_to(keep[None], (30, 8, 256)), 0.0)
        keep_s[m * 240 : (m + 1) * 240, :] = mm(pick.reshape(240, 256).astype(bf16), ones)
    feed_forward(w1_ref, b1_ref, w2_ref, x_s, acc_s, act_s, w1_s, w2_s, sem, x_s.shape[0])
    emb = finish_rows(slice(0, Q_ROWS), acc_s, gain, nbias, proj_ref, hidden_ref, projected_ref).astype(bf16)
    row = lax.broadcasted_iota(i32, (16, EMB), 0)
    token = lax.broadcasted_iota(i32, (16, EMB), 1) + EMB * (row % 2)
    owner = token // q_len
    slot = token % q_len
    lens = jnp.zeros((16, EMB), i32)
    posi = jnp.zeros((16, EMB), i32)
    for q in range(q_dev):
        lens = jnp.where(owner == q, qlen_ref[q], lens)
        posi = jnp.where(owner == q, pos_ref[q], posi)
    kept = jnp.where(slot < lens, 1.0, 0.0)
    meta = jnp.where(row < 2, kept, jnp.where(row < 4, posi.astype(f32), 0.0)).astype(bf16)
    for k in range(YZ_PEERS):
        qsend_ref[k, 0:Q_ROWS, :] = emb
        qsend_ref[k, Q_ROWS : Q_ROWS + 16, :] = meta
    for m in range(3):
        r = slice(Q_ROWS + m * 240, Q_ROWS + (m + 1) * 240)
        normed = finish_rows(r, acc_s, gain, nbias, proj_ref, hidden_ref, projected_ref)
        r = slice(m * 240, (m + 1) * 240)
        psend_ref[r, :] = jnp.where(keep_s[r, :] > 0.5, normed, MASKED).astype(bf16)


def encode(xq, xp, qlen, plen, ids, pos, w1, b1, w2, b2, gain, nbias, proj):
    width, ff = w1.shape
    count = ff // FCHUNK
    rows = Q_ROWS + P_ROWS
    far = pl.BlockSpec(memory_space=pltpu.HBM)
    return pl.pallas_call(
        encode_kernel,
        in_specs=[SM, SM, SM, VM, VM, VM, far, VM, far, VM, VM, VM, VM],
        out_specs=[VM] * 4,
        out_shape=[
            jax.ShapeDtypeStruct((rows, width), bf16),
            jax.ShapeDtypeStruct((rows, EMB), f32),
            jax.ShapeDtypeStruct((YZ_PEERS, Q_ROWS + 16, EMB), bf16),
            jax.ShapeDtypeStruct((P_ROWS, EMB), bf16),
        ],
        scratch_shapes=[
            pltpu.VMEM((rows, width), bf16),
            pltpu.VMEM((rows, width), f32),
            pltpu.VMEM((2, rows, FCHUNK), bf16),
            pltpu.VMEM((count, width, FCHUNK), bf16),
            pltpu.VMEM((count, FCHUNK, width), bf16),
            pltpu.SemaphoreType.DMA((2, count)),
            pltpu.VMEM((P_ROWS, EMB), f32),
            pltpu.VMEM((8, 256), i32),
        ],
        compiler_params=pltpu.CompilerParams(vmem_limit_bytes=60 << 20),
        cost_estimate=pl.CostEstimate(flops=4 * rows * width * ff, bytes_accessed=4 * width * ff, transcendentals=rows * ff),
        name="encode",
    )(qlen, pos, plen, ids, xq, xp, w1, b1[None], w2, b2, gain, nbias, proj)


def load_pairs(q_ref, p_refs, qt_s, pa_s, keep_s):
    for k in range(YZ_PEERS):
        qt_s[0:EMB, k * 256 : (k + 1) * 256] = q_ref[k, 0:Q_ROWS, :].T
        for h in range(2):
            keep_s[:, k * 256 + h * 128 : k * 256 + (h + 1) * 128] = q_ref[k, 256 + h : 257 + h, :].astype(f32)
    cols = qt_s.shape[1]
    first = lax.broadcasted_iota(i32, (EMB, cols), 0) == 0
    qt_s[EMB : 2 * EMB, :] = jnp.where(first, 1.0, 0.0).astype(bf16)
    for k, p_ref in enumerate(p_refs):
        r = slice(k * P_ROWS, (k + 1) * P_ROWS)
        val = p_ref[...]
        pa_s[r, 0:EMB] = val
        pa_s[r, EMB : 2 * EMB] = jnp.where(val.astype(f32) > 1.5, BIAS, 0.0).astype(bf16)


def forward_kernel(q_ref, *refs):
    p_refs = refs[:X_PEERS]
    sc_ref, tot_ref, zsend_ref, qt_s, pa_s, keep_s, sum_s = refs[X_PEERS:]
    load_pairs(q_ref, p_refs, qt_s, pa_s, keep_s)
    cols = qt_s.shape[1]

    def group(g, carry):
        for j in range(cols // 256):
            c = slice(j * 256, (j + 1) * 256)
            total = jnp.zeros((8, 256), f32)
            for m in range(3):
                r = pl.ds(pl.multiple_of(g * P_ROWS + m * 240, 16), 240)
                e = jnp.exp2(mm(pa_s[r, :], qt_s[:, c]) * SCALE)
                total = total + jnp.sum(e.reshape(30, 8, 256), axis=0)
            sum_s[pl.ds(pl.multiple_of(g * 8, 8), 8), c] = total
        return carry

    lax.fori_loop(0, X_PEERS, group, 0)
    for g in range(X_PEERS):
        tot_ref[4 * g : 4 * g + 4, :] = sum_s[8 * g : 8 * g + 4, :] + sum_s[8 * g + 4 : 8 * g + 8, :]
    a = lax.broadcasted_iota(i32, (128, 128), 0) // 32
    b = lax.broadcasted_iota(i32, (128, 128), 1) // 32
    same = jnp.where(a == b, 1.0, 0.0)
    for t in range(cols // 128):
        c = slice(t * 128, (t + 1) * 128)
        soft = jnp.log(tot_ref[:, c]) * temper * keep_s[:, c]
        sc = jnp.dot(soft, same, preferred_element_type=f32, precision=lax.Precision.HIGHEST)
        sc_ref[:, c] = sc
        z = jnp.sum(jnp.exp(sc), axis=0, keepdims=True)
        for k in range(YZ_PEERS):
            zsend_ref[k, t : t + 1, :] = z


def forward(q, ps):
    cols = YZ_PEERS * Q_ROWS
    return pl.pallas_call(
        forward_kernel,
        in_specs=[VM] * (1 + X_PEERS),
        out_specs=[VM] * 3,
        out_shape=[
            jax.ShapeDtypeStruct((16, cols), f32),
            jax.ShapeDtypeStruct((16, cols), f32),
            jax.ShapeDtypeStruct((YZ_PEERS, 16, 128), f32),
        ],
        scratch_shapes=[
            pltpu.VMEM((256, cols), bf16),
            pltpu.VMEM((X_PEERS * P_ROWS, 256), bf16),
            pltpu.VMEM((1, cols), f32),
            pltpu.VMEM((8 * X_PEERS, cols), f32),
        ],
        compiler_params=pltpu.CompilerParams(vmem_limit_bytes=16 << 20),
        name="pair_forward",
    )(q, *ps)


def backward_kernel(me_ref, q_ref, *refs):
    p_refs = refs[:X_PEERS]
    sc_ref, tot_ref, z_ref = refs[X_PEERS : X_PEERS + 3]
    dp_refs = refs[X_PEERS + 3 : 2 * X_PEERS + 3]
    dq_ref, loss_ref, qt_s, pa_s, keep_s, pt_s, q_s, fac_s, g_s, dp_s = refs[2 * X_PEERS + 3 :]
    load_pairs(q_ref, p_refs, qt_s, pa_s, keep_s)
    cols = qt_s.shape[1]
    p_all = pa_s.shape[0]
    for i in range(0, p_all, 128):
        n = min(128, p_all - i)
        pt_s[:, i : i + n] = pa_s[i : i + n, 0:EMB].T
    for k in range(YZ_PEERS):
        q_s[k * 256 : (k + 1) * 256, :] = q_ref[k, 0:Q_ROWS, :]
    me = me_ref[0]
    x = me % X_PEERS
    row = lax.broadcasted_iota(i32, (16, 128), 0)
    number = row % 4 + (me // X_PEERS) * 16
    for k in range(X_PEERS):
        number = jnp.where(row // 4 == k, number + ((x + X_PEERS - k) % X_PEERS) * 4, number)
    number = number.astype(f32)
    lane = lax.broadcasted_iota(i32, (1, 128), 1)
    head = jnp.where(lane % 32 == 0, 1.0, 0.0)
    loss = jnp.zeros((1, 128), f32)
    for t in range(cols // 128):
        c = slice(t * 128, (t + 1) * 128)
        z = z_ref[0, t : t + 1, :]
        for k in range(1, YZ_PEERS):
            z = z + z_ref[k, t : t + 1, :]
        sc = sc_ref[:, c]
        pos = q_ref[t // 2, 258 + t % 2 : 259 + t % 2, :].astype(f32)
        hit = jnp.where(number == pos, 1.0, 0.0)
        fac = (jnp.exp(sc) / z - hit) * (keep_s[:, c] / tot_ref[:, c])
        for g in range(X_PEERS):
            fac_s[8 * g : 8 * g + 4, c] = fac[4 * g : 4 * g + 4, :]
            fac_s[8 * g + 4 : 8 * g + 8, c] = fac[4 * g : 4 * g + 4, :]
        loss = loss + (jnp.log(z) * (1.0 / YZ_PEERS) - jnp.sum(hit * sc, axis=0, keepdims=True)) * head
    loss_ref[...] = jnp.broadcast_to(jnp.sum(loss, axis=1, keepdims=True), loss_ref.shape)

    wide = g_s.shape[1]

    def columns(j, carry):
        base = pl.multiple_of(j * wide, wide)

        def group(g, carry):
            for m in range(3):
                r = pl.ds(pl.multiple_of(g * P_ROWS + m * 240, 16), 240)
                lhs = pa_s[r, :]
                for h in range(wide // 256):
                    c = pl.ds(base + h * 256, 256)
                    e = jnp.exp2(mm(lhs, qt_s[:, c]) * SCALE)
                    fac = fac_s[pl.ds(pl.multiple_of(g * 8, 8), 8), c]
                    grad = e.reshape(30, 8, 256) * fac[None]
                    g_s[r, h * 256 : (h + 1) * 256] = grad.reshape(240, 256).astype(bf16)
            return carry

        lax.fori_loop(0, X_PEERS, group, 0)
        dq = mm(pt_s[...], g_s[...]).astype(bf16)
        for h in range(wide // 256):
            dq_ref[pl.ds(j * (wide // 256) + h, 1)] = dq[None, :, h * 256 : (h + 1) * 256]
        qb = q_s[pl.ds(base, wide), :]

        def rows(m, carry):
            r = pl.ds(pl.multiple_of(m * P_ROWS, 16), P_ROWS)
            part = mm(g_s[r, :], qb)
            dp_s[r, :] = jnp.where(j == 0, part, dp_s[r, :] + part)
            return carry

        lax.fori_loop(0, X_PEERS, rows, 0)
        return carry

    lax.fori_loop(0, cols // wide, columns, 0)
    for k in range(X_PEERS):
        dp_refs[k][...] = dp_s[k * P_ROWS : (k + 1) * P_ROWS, :].astype(dp_refs[k].dtype)


def backward(me, q, ps, sc, tot, z):
    cols = YZ_PEERS * Q_ROWS
    p_all = X_PEERS * P_ROWS
    wide = 512
    out = pl.pallas_call(
        backward_kernel,
        in_specs=[SM] + [VM] * (X_PEERS + 4),
        out_specs=[VM] * (X_PEERS + 2),
        out_shape=[jax.ShapeDtypeStruct((P_ROWS, EMB), f32 if k == 0 else bf16) for k in range(X_PEERS)]
        + [
            jax.ShapeDtypeStruct((YZ_PEERS, EMB, Q_ROWS), bf16),
            jax.ShapeDtypeStruct((1, 128), f32),
        ],
        scratch_shapes=[
            pltpu.VMEM((256, cols), bf16),
            pltpu.VMEM((p_all, 256), bf16),
            pltpu.VMEM((1, cols), f32),
            pltpu.VMEM((EMB, p_all), bf16),
            pltpu.VMEM((cols, EMB), bf16),
            pltpu.VMEM((8 * X_PEERS, cols), f32),
            pltpu.VMEM((p_all, wide), bf16),
            pltpu.VMEM((p_all, EMB), f32),
        ],
        compiler_params=pltpu.CompilerParams(vmem_limit_bytes=20 << 20),
        name="pair_backward",
    )(me, q, *ps, sc, tot, z)
    return out[:X_PEERS], out[X_PEERS], out[X_PEERS + 1]


def final_kernel(*refs):
    dp_refs = refs[:X_PEERS]
    dq_ref, projected_ref, hidden_ref, loss_ref, pgrad_ref, share_ref, bt_s, bp_s, share_s = refs[X_PEERS:]
    pr = projected_ref[0:Q_ROWS, :]
    inv = lax.rsqrt(jnp.sum(pr * pr, -1, keepdims=True) + eps_norm)
    nt = (pr * inv).T
    it = jnp.broadcast_to(inv, pr.shape).T
    grad = dq_ref[0].astype(f32)
    for k in range(1, YZ_PEERS):
        grad = grad + dq_ref[k].astype(f32)
    dot = jnp.sum(nt * grad, axis=0, keepdims=True)
    bt_s[...] = (it * (grad - nt * dot)).astype(bf16)
    for m in range(3):
        r = slice(m * 240, (m + 1) * 240)
        grad = dp_refs[0][r, :].astype(f32)
        for k in range(1, X_PEERS):
            grad = grad + dp_refs[k][r, :].astype(f32)
        pgrad_ref[r, :] = grad
        pr = projected_ref[Q_ROWS + m * 240 : Q_ROWS + (m + 1) * 240, :]
        inv = lax.rsqrt(jnp.sum(pr * pr, -1, keepdims=True) + eps_norm)
        nm = pr * inv
        bp_s[r, :] = inv * (grad - nm * jnp.sum(nm * grad, -1, keepdims=True))
    bpt = bp_s[...].T.astype(bf16)
    for k in range(6):
        c = slice(k * 128, (k + 1) * 128)
        pg = mm(bt_s[...], hidden_ref[0:Q_ROWS, c]) + mm(bpt, hidden_ref[Q_ROWS:, c])
        share_s[:, k, :] = pg.T
    loss = loss_ref[...]
    high = loss.astype(bf16).astype(f32)
    share_s[:, 6, :] = jnp.broadcast_to(high, (128, 128))
    share_s[:, 7, :] = jnp.broadcast_to(loss - high, (128, 128))
    share_ref[...] = share_s[...].astype(bf16)


def final(dps, dq, projected, hidden, loss):
    return pl.pallas_call(
        final_kernel,
        in_specs=[VM] * (X_PEERS + 4),
        out_specs=[VM] * 2,
        out_shape=[
            jax.ShapeDtypeStruct((P_ROWS, EMB), f32),
            jax.ShapeDtypeStruct((128, 8, 128), bf16),
        ],
        scratch_shapes=[
            pltpu.VMEM((EMB, Q_ROWS), bf16),
            pltpu.VMEM((P_ROWS, EMB), f32),
            pltpu.VMEM((128, 8, 128), f32),
        ],
        compiler_params=pltpu.CompilerParams(vmem_limit_bytes=12 << 20),
        name="final_grad",
    )(*dps, dq, projected, hidden, loss)


def x_ring(k):
    return [(j, (j // 4) * 4 + (j % 4 + k) % 4) for j in range(32)]


def inverse(pairs):
    return [(b, a) for a, b in pairs]


def per_device(
    query_states, passage_states, query_lengths, passage_lengths, passage_ids, positives,
    up_weight, up_bias, down_weight, down_bias, norm_gain, norm_bias, proj_weight,
):
    p_dev, p_len, _ = passage_states.shape
    queries = query_states.shape[0] * lax.axis_size("rep") * lax.axis_size("dp")
    me = lax.axis_index("dp").reshape(1)
    yz_groups = [[4 * k + i for k in range(YZ_PEERS)] for i in range(X_PEERS)]

    hidden, projected, qsend, psend = encode(
        query_states, jnp.swapaxes(passage_states, 0, 1), query_lengths, passage_lengths, passage_ids,
        positives, up_weight, up_bias, down_weight, down_bias, norm_gain, norm_bias, proj_weight,
    )
    q = lax.all_to_all(qsend, "dp", 0, 0, axis_index_groups=yz_groups, tiled=True)
    ps = [psend] + [lax.ppermute(psend, "dp", x_ring(k)) for k in range(1, X_PEERS)]
    sc, tot, zsend = forward(q, ps)
    z = lax.all_to_all(zsend, "dp", 0, 0, axis_index_groups=yz_groups, tiled=True)
    dps, dqs, loss = backward(me, q, ps, sc, tot, z)
    dps = [dps[0]] + [lax.ppermute(dps[k], "dp", inverse(x_ring(k))) for k in range(1, X_PEERS)]
    dq = lax.all_to_all(dqs, "dp", 0, 0, axis_index_groups=yz_groups, tiled=True)
    pgrad, share = final(dps, dq, projected, hidden, loss)
    passage_grad = jnp.swapaxes(pgrad.reshape(p_len, p_dev, EMB), 0, 1)
    parts = lax.all_to_all(share, ("rep", "dp"), 0, 0, tiled=True)
    summed = jnp.sum(parts.astype(f32), axis=0)
    mean_loss = (summed[6, 0] + summed[7, 0]) / queries
    out = jnp.broadcast_to(summed.astype(bf16)[None], parts.shape)
    pieces = lax.all_to_all(out, ("rep", "dp"), 0, 0, tiled=True)
    proj_grad = jnp.swapaxes(pieces[:, :6, :], 0, 1).reshape(768, 128).astype(f32)
    return (mean_loss, passage_grad, proj_grad)


def solution(mesh):
    rows = P(("rep", "dp"))
    in_specs = (rows,) * 6 + (P(),) * 7
    out_specs = (P(), rows, P())
    return jax.shard_map(
        per_device, mesh=mesh, in_specs=in_specs, out_specs=out_specs, check_vma=False
    )
```

```python
import jax
import jax.numpy as jnp
from jax import lax
from jax.experimental import pallas as pl
from jax.experimental.pallas import tpu as pltpu
from jax.sharding import PartitionSpec as P

temper = 0.05
eps_norm = 1e-06
punct_low = 999
punct_high = 1067

bf16 = jnp.bfloat16
f32 = jnp.float32
i32 = jnp.int32


X_PEERS = 4
YZ_PEERS = 8
P_ROWS = 720
Q_ROWS = 256
EMB = 128
FCHUNK = 1024
MASKED = 2.0
BIAS = -10000.0
SCALE = 1.4426950408889634 / temper

VM = pl.BlockSpec(memory_space=pltpu.VMEM)
SM = pl.BlockSpec(memory_space=pltpu.SMEM)


def mm(a, b):
    return jnp.dot(a, b, preferred_element_type=f32)


def fetch(which, k, w1_ref, w2_ref, w1_s, w2_s, sem):
    c = pl.ds(pl.multiple_of(k * FCHUNK, FCHUNK), FCHUNK)
    if which == 0:
        return pltpu.make_async_copy(w1_ref.at[:, c], w1_s.at[k], sem.at[0, k])
    return pltpu.make_async_copy(w2_ref.at[c, :], w2_s.at[k], sem.at[1, k])


def feed_forward(w1_ref, b1_s, w2_ref, x_s, acc_s, act_s, w1_s, w2_s, sem):
    count = w1_s.shape[0]

    def step(k, carry):
        fetch(0, k, w1_ref, w2_ref, w1_s, w2_s, sem).wait()

        @pl.when(k + 1 < count)
        def _():
            fetch(0, k + 1, w1_ref, w2_ref, w1_s, w2_s, sem).start()
            fetch(1, k + 1, w1_ref, w2_ref, w1_s, w2_s, sem).start()

        bias = b1_s[:, pl.ds(pl.multiple_of(k * FCHUNK, FCHUNK), FCHUNK)]
        up = mm(x_s[...], w1_s[k]) + bias
        act_s[...] = (up * 0.5 * (1.0 + lax.erf(up * 0.7071067811865476))).astype(bf16)
        fetch(1, k, w1_ref, w2_ref, w1_s, w2_s, sem).wait()
        acc_s[...] += mm(act_s[...], w2_s[k])
        return carry

    lax.fori_loop(0, count, step, 0)


def finish_rows(r, acc_s, gain, nbias, proj_ref, hidden_ref, projected_ref):
    width = acc_s.shape[1]
    res = acc_s[r, :]
    mean = jnp.sum(res, -1, keepdims=True) * (1.0 / width)
    cen = res - mean
    var = jnp.sum(cen * cen, -1, keepdims=True) * (1.0 / width)
    hid = (cen * lax.rsqrt(var + eps_norm) * gain + nbias).astype(bf16)
    hidden_ref[r, :] = hid
    pr = mm(hid, proj_ref[...])
    projected_ref[r, :] = pr
    return pr * lax.rsqrt(jnp.sum(pr * pr, -1, keepdims=True) + eps_norm)


def encode_kernel(
    qlen_any, pos_any, plen_any, ids_any, xq_any, xp_any, w1_ref, b1_any, w2_ref, b2_any,
    gain_any, nbias_any, proj_any, hidden_ref, projected_ref, qsend_ref, psend_ref,
    x_s, acc_s, act_s, w1_s, w2_s, sem, keep_s, ids_s, small_sem,
    qlen_ref, pos_ref, plen_ref, ids_ref, xq_ref, xp_ref, b1_ref, b2_ref, gain_ref, nbias_ref, proj_ref,
):
    sources = (xp_any, xq_any, b2_any, ids_any, plen_any, b1_any, gain_any, nbias_any, proj_any, qlen_any, pos_any)
    targets = (xp_ref, xq_ref, b2_ref, ids_ref, plen_ref, b1_ref, gain_ref, nbias_ref, proj_ref, qlen_ref, pos_ref)
    fetch(0, 0, w1_ref, w2_ref, w1_s, w2_s, sem).start()
    copies = [pltpu.make_async_copy(a, b, small_sem.at[i]) for i, (a, b) in enumerate(zip(sources, targets))]
    for copy in copies:
        copy.start()
    fetch(1, 0, w1_ref, w2_ref, w1_s, w2_s, sem).start()
    q_dev, q_len, width = xq_ref.shape
    p_len, p_dev, _ = xp_ref.shape
    for copy in copies:
        copy.wait()
    b2, gain, nbias = (v[...].reshape(1, width) for v in (b2_ref, gain_ref, nbias_ref))
    x_s[0:Q_ROWS, :] = xq_ref[...].reshape(Q_ROWS, width)
    x_s[Q_ROWS:, :] = xp_ref[...].reshape(P_ROWS, width)
    acc_s[...] = x_s[...].astype(f32) + b2
    ids_s[...] = jnp.zeros_like(ids_s)
    ids_s[0:p_dev, 0:p_len] = ids_ref[...]
    ids_s[p_dev : 2 * p_dev, 0:p_len] = ids_ref[...]
    ids = ids_s[...]
    row = lax.broadcasted_iota(i32, (8, 256), 0) % p_dev
    col = lax.broadcasted_iota(i32, (8, 256), 1)
    lens = jnp.zeros((8, 256), i32)
    for p in range(p_dev):
        lens = jnp.where(row == p, plen_ref[p], lens)
    punct = jnp.logical_and(ids >= punct_low, ids < punct_high)
    keep = jnp.where(jnp.logical_and(col < lens, jnp.logical_not(punct)), 1.0, 0.0)
    ones = jnp.ones((256, EMB), bf16)
    slab = lax.broadcasted_iota(i32, (30, 8, 256), 0) * 2 + lax.broadcasted_iota(i32, (30, 8, 256), 1) // p_dev
    cols = lax.broadcasted_iota(i32, (30, 8, 256), 2)
    for m in range(3):
        pick = jnp.where(slab + m * 60 == cols, jnp.broadcast_to(keep[None], (30, 8, 256)), 0.0)
        keep_s[m * 240 : (m + 1) * 240, :] = mm(pick.reshape(240, 256).astype(bf16), ones)
    feed_forward(w1_ref, b1_ref, w2_ref, x_s, acc_s, act_s, w1_s, w2_s, sem)
    emb = finish_rows(slice(0, Q_ROWS), acc_s, gain, nbias, proj_ref, hidden_ref, projected_ref).astype(bf16)
    row = lax.broadcasted_iota(i32, (16, EMB), 0)
    token = lax.broadcasted_iota(i32, (16, EMB), 1) + EMB * (row % 2)
    owner = token // q_len
    slot = token % q_len
    lens = jnp.zeros((16, EMB), i32)
    posi = jnp.zeros((16, EMB), i32)
    for q in range(q_dev):
        lens = jnp.where(owner == q, qlen_ref[q], lens)
        posi = jnp.where(owner == q, pos_ref[q], posi)
    kept = jnp.where(slot < lens, 1.0, 0.0)
    meta = jnp.where(row < 2, kept, jnp.where(row < 4, posi.astype(f32), 0.0)).astype(bf16)
    qsend_ref[0:Q_ROWS, :] = emb
    qsend_ref[Q_ROWS : Q_ROWS + 16, :] = meta
    for m in range(3):
        r = slice(Q_ROWS + m * 240, Q_ROWS + (m + 1) * 240)
        normed = finish_rows(r, acc_s, gain, nbias, proj_ref, hidden_ref, projected_ref)
        r = slice(m * 240, (m + 1) * 240)
        psend_ref[r, :] = jnp.where(keep_s[r, :] > 0.5, normed, MASKED).astype(bf16)


def encode(xq, xp, qlen, plen, ids, pos, w1, b1, w2, b2, gain, nbias, proj):
    width, ff = w1.shape
    count = ff // FCHUNK
    rows = Q_ROWS + P_ROWS
    far = pl.BlockSpec(memory_space=pltpu.HBM)
    return pl.pallas_call(
        encode_kernel,
        in_specs=[far] * 13,
        out_specs=[VM] * 4,
        out_shape=[
            jax.ShapeDtypeStruct((rows, width), bf16),
            jax.ShapeDtypeStruct((rows, EMB), f32),
            jax.ShapeDtypeStruct((Q_ROWS + 16, EMB), bf16),
            jax.ShapeDtypeStruct((P_ROWS, EMB), bf16),
        ],
        scratch_shapes=[
            pltpu.VMEM((rows, width), bf16),
            pltpu.VMEM((rows, width), f32),
            pltpu.VMEM((rows, FCHUNK), bf16),
            pltpu.VMEM((count, width, FCHUNK), bf16),
            pltpu.VMEM((count, FCHUNK, width), bf16),
            pltpu.SemaphoreType.DMA((2, count)),
            pltpu.VMEM((P_ROWS, EMB), f32),
            pltpu.VMEM((8, 256), i32),
            pltpu.SemaphoreType.DMA((11,)),
            pltpu.SMEM(qlen.shape, i32),
            pltpu.SMEM(pos.shape, i32),
            pltpu.SMEM(plen.shape, i32),
            pltpu.VMEM(ids.shape, i32),
            pltpu.VMEM(xq.shape, bf16),
            pltpu.VMEM(xp.shape, bf16),
            pltpu.VMEM((1, ff), f32),
            pltpu.VMEM((width,), f32),
            pltpu.VMEM((width,), f32),
            pltpu.VMEM((width,), f32),
            pltpu.VMEM(proj.shape, bf16),
        ],
        cost_estimate=pl.CostEstimate(flops=4 * rows * width * ff, bytes_accessed=4 * width * ff, transcendentals=rows * ff),
        name="encode",
    )(qlen, pos, plen, ids, xq, xp, w1, b1[None], w2, b2, gain, nbias, proj)


def load_pairs(q_refs, p_refs, qt_s, pa_s, keep_s):
    for k in range(YZ_PEERS):
        q_ref = q_refs[k // 2]
        qt_s[0:EMB, k * 256 : (k + 1) * 256] = q_ref[k % 2, 0:Q_ROWS, :].T
        for h in range(2):
            keep_s[:, k * 256 + h * 128 : k * 256 + (h + 1) * 128] = q_ref[k % 2, 256 + h : 257 + h, :].astype(f32)
    cols = qt_s.shape[1]
    first = lax.broadcasted_iota(i32, (EMB, cols), 0) == 0
    qt_s[EMB : 2 * EMB, :] = jnp.where(first, 1.0, 0.0).astype(bf16)
    for k, p_ref in enumerate(p_refs):
        r = slice(k * P_ROWS, (k + 1) * P_ROWS)
        val = p_ref[...]
        pa_s[r, 0:EMB] = val
        pa_s[r, EMB : 2 * EMB] = jnp.where(val.astype(f32) > 1.5, BIAS, 0.0).astype(bf16)


def origin(me, block):
    yz = me // X_PEERS
    y = (yz // 4 + block % 2) % 2
    return y * 4 + (yz % 4 + 4 - block // 2) % 4


def forward_kernel(me_ref, *refs):
    q_refs, p_refs = refs[:4], refs[4 : 4 + X_PEERS]
    sc_ref, tot_ref, zpart_ref, e_ref, qt_s, pa_s, keep_s, sum_s = refs[4 + X_PEERS :]
    load_pairs(q_refs, p_refs, qt_s, pa_s, keep_s)
    cols = qt_s.shape[1]

    def group(g, carry):
        for j in range(cols // 256):
            c = slice(j * 256, (j + 1) * 256)
            total = jnp.zeros((8, 256), f32)
            for m in range(3):
                r = pl.ds(pl.multiple_of(g * P_ROWS + m * 240, 16), 240)
                e = jnp.exp2(mm(pa_s[r, :], qt_s[:, c]) * SCALE)
                e_ref[r, c] = e.astype(bf16)
                total = total + jnp.sum(e.reshape(30, 8, 256), axis=0)
            sum_s[pl.ds(pl.multiple_of(g * 8, 8), 8), c] = total
        return carry

    lax.fori_loop(0, X_PEERS, group, 0)
    for g in range(X_PEERS):
        tot_ref[4 * g : 4 * g + 4, :] = sum_s[8 * g : 8 * g + 4, :] + sum_s[8 * g + 4 : 8 * g + 8, :]
    a = lax.broadcasted_iota(i32, (128, 128), 0) // 32
    b = lax.broadcasted_iota(i32, (128, 128), 1) // 32
    same = jnp.where(a == b, 1.0, 0.0)
    for t in range(cols // 128):
        c = slice(t * 128, (t + 1) * 128)
        soft = jnp.log(tot_ref[:, c]) * temper * keep_s[:, c]
        sc = jnp.dot(soft, same, preferred_element_type=f32, precision=lax.Precision.HIGHEST)
        sc_ref[:, c] = sc
        z = jnp.sum(jnp.exp(sc), axis=0, keepdims=True)
        zpart_ref[pl.ds(origin(me_ref[0], t // 2) * 2 + t % 2, 1), :] = z


def forward(me, qs, ps):
    cols = YZ_PEERS * Q_ROWS
    return pl.pallas_call(
        forward_kernel,
        in_specs=[SM] + [VM] * (4 + X_PEERS),
        out_specs=[VM] * 4,
        out_shape=[
            jax.ShapeDtypeStruct((16, cols), f32),
            jax.ShapeDtypeStruct((16, cols), f32),
            jax.ShapeDtypeStruct((16, 128), f32),
            jax.ShapeDtypeStruct((X_PEERS * P_ROWS, cols), bf16),
        ],
        scratch_shapes=[
            pltpu.VMEM((256, cols), bf16),
            pltpu.VMEM((X_PEERS * P_ROWS, 256), bf16),
            pltpu.VMEM((1, cols), f32),
            pltpu.VMEM((8 * X_PEERS, cols), f32),
        ],
        compiler_params=pltpu.CompilerParams(vmem_limit_bytes=16 << 20),
        name="pair_forward",
    )(me, *qs, *ps)


def backward_kernel(me_ref, *refs):
    q_refs, p_refs, refs = refs[:4], refs[4 : 4 + X_PEERS], refs[4 + X_PEERS :]
    sc_ref, tot_ref, za_ref, zb_ref, e_ref = refs[:5]
    dp_refs, dq_refs, refs = refs[5 : 5 + X_PEERS], refs[5 + X_PEERS : 9 + X_PEERS], refs[9 + X_PEERS :]
    loss_ref, p_s, pt_s, q_s, fac_s, g_s, dp_s = refs
    p_all, cols = g_s.shape
    for k, p_ref in enumerate(p_refs):
        p_s[k * P_ROWS : (k + 1) * P_ROWS, :] = p_ref[...]
    for i in range(0, p_all, 128):
        n = min(128, p_all - i)
        pt_s[:, i : i + n] = p_s[i : i + n, :].T
    for k in range(YZ_PEERS):
        q_s[k * 256 : (k + 1) * 256, :] = q_refs[k // 2][k % 2, 0:Q_ROWS, :]
    me = me_ref[0]
    x = me % X_PEERS
    row = lax.broadcasted_iota(i32, (16, 128), 0)
    number = row % 4 + (me // X_PEERS) * 16
    for k in range(X_PEERS):
        number = jnp.where(row // 4 == k, number + ((x + X_PEERS - k) % X_PEERS) * 4, number)
    number = number.astype(f32)
    lane = lax.broadcasted_iota(i32, (1, 128), 1)
    head = jnp.where(lane % 32 == 0, 1.0, 0.0)
    loss = jnp.zeros((1, 128), f32)
    for t in range(cols // 128):
        c = slice(t * 128, (t + 1) * 128)
        at = pl.ds(origin(me, t // 2) * 2 + t % 2, 1)
        z = za_ref[at, :] + zb_ref[at, :]
        sc = sc_ref[:, c]
        q_ref, a = q_refs[t // 4], t // 2 % 2
        keep = q_ref[a, 256 + t % 2 : 257 + t % 2, :].astype(f32)
        pos = q_ref[a, 258 + t % 2 : 259 + t % 2, :].astype(f32)
        hit = jnp.where(number == pos, 1.0, 0.0)
        fac = (jnp.exp(sc) / z - hit) * (keep / tot_ref[:, c])
        for g in range(X_PEERS):
            fac_s[8 * g : 8 * g + 4, c] = fac[4 * g : 4 * g + 4, :]
            fac_s[8 * g + 4 : 8 * g + 8, c] = fac[4 * g : 4 * g + 4, :]
        loss = loss + (jnp.log(z) * (1.0 / YZ_PEERS) - jnp.sum(hit * sc, axis=0, keepdims=True)) * head
    loss_ref[...] = jnp.broadcast_to(jnp.sum(loss, axis=1, keepdims=True), loss_ref.shape)

    def group(g, carry):
        for m in range(3):
            r = pl.ds(pl.multiple_of(g * P_ROWS + m * 240, 16), 240)
            for j in range(cols // 256):
                c = slice(j * 256, (j + 1) * 256)
                fac = fac_s[pl.ds(pl.multiple_of(g * 8, 8), 8), c]
                grad = e_ref[r, c].astype(f32).reshape(30, 8, 256) * fac[None]
                g_s[r, c] = grad.reshape(240, 256).astype(bf16)
            dp_s[r, :] = mm(g_s[r, :], q_s[...])
        return carry

    lax.fori_loop(0, X_PEERS, group, 0)

    for k in range(4):
        dq = mm(pt_s[...], g_s[:, k * 512 : (k + 1) * 512]).astype(bf16)
        for h in range(2):
            dq_refs[k][h] = dq[:, h * 256 : (h + 1) * 256]
    for k in range(X_PEERS):
        dp_refs[k][...] = dp_s[k * P_ROWS : (k + 1) * P_ROWS, :].astype(dp_refs[k].dtype)


def backward(me, qs, ps, sc, tot, za, zb, e):
    p_all, cols = e.shape
    out = pl.pallas_call(
        backward_kernel,
        in_specs=[SM] + [VM] * (X_PEERS + 9),
        out_specs=[VM] * (X_PEERS + 5),
        out_shape=[jax.ShapeDtypeStruct((P_ROWS, EMB), f32 if k == 0 else bf16) for k in range(X_PEERS)]
        + [jax.ShapeDtypeStruct((2, EMB, Q_ROWS), bf16)] * 4
        + [jax.ShapeDtypeStruct((1, 128), f32)],
        scratch_shapes=[
            pltpu.VMEM((p_all, EMB), bf16),
            pltpu.VMEM((EMB, p_all), bf16),
            pltpu.VMEM((cols, EMB), bf16),
            pltpu.VMEM((8 * X_PEERS, cols), f32),
            pltpu.VMEM((p_all, cols), bf16),
            pltpu.VMEM((p_all, EMB), f32),
        ],
        compiler_params=pltpu.CompilerParams(vmem_limit_bytes=24 << 20),
        name="pair_backward",
    )(me, *qs, *ps, sc, tot, za, zb, e)
    return out[:X_PEERS], out[X_PEERS : X_PEERS + 4], out[-1]


def final_kernel(*refs):
    dp_refs = refs[:X_PEERS]
    dqa_ref, dqb_ref, projected_ref, hidden_ref, loss_ref, pgrad_ref, share_ref, bt_s, bp_s, share_s = refs[X_PEERS:]
    pr = projected_ref[0:Q_ROWS, :]
    inv = lax.rsqrt(jnp.sum(pr * pr, -1, keepdims=True) + eps_norm)
    nt = (pr * inv).T
    it = jnp.broadcast_to(inv, pr.shape).T
    grad = dqa_ref[...] + dqb_ref[...].astype(f32)
    dot = jnp.sum(nt * grad, axis=0, keepdims=True)
    bt_s[...] = (it * (grad - nt * dot)).astype(bf16)
    for m in range(3):
        r = slice(m * 240, (m + 1) * 240)
        grad = dp_refs[0][r, :].astype(f32)
        for k in range(1, X_PEERS):
            grad = grad + dp_refs[k][r, :].astype(f32)
        pgrad_ref[r, :] = grad
        pr = projected_ref[Q_ROWS + m * 240 : Q_ROWS + (m + 1) * 240, :]
        inv = lax.rsqrt(jnp.sum(pr * pr, -1, keepdims=True) + eps_norm)
        nm = pr * inv
        bp_s[r, :] = inv * (grad - nm * jnp.sum(nm * grad, -1, keepdims=True))
    bpt = bp_s[...].T.astype(bf16)
    for k in range(6):
        c = slice(k * 128, (k + 1) * 128)
        pg = mm(bt_s[...], hidden_ref[0:Q_ROWS, c]) + mm(bpt, hidden_ref[Q_ROWS:, c])
        share_s[:, k, :] = pg.T
    loss = loss_ref[...]
    high = loss.astype(bf16).astype(f32)
    share_s[:, 6, :] = jnp.broadcast_to(high, (128, 128))
    share_s[:, 7, :] = jnp.broadcast_to(loss - high, (128, 128))
    share_ref[...] = share_s[...].astype(bf16)


def final(dps, dqa, dqb, projected, hidden, loss):
    return pl.pallas_call(
        final_kernel,
        in_specs=[VM] * (X_PEERS + 5),
        out_specs=[VM] * 2,
        out_shape=[
            jax.ShapeDtypeStruct((P_ROWS, EMB), f32),
            jax.ShapeDtypeStruct((128, 8, 128), bf16),
        ],
        scratch_shapes=[
            pltpu.VMEM((EMB, Q_ROWS), bf16),
            pltpu.VMEM((P_ROWS, EMB), f32),
            pltpu.VMEM((128, 8, 128), f32),
        ],
        compiler_params=pltpu.CompilerParams(vmem_limit_bytes=12 << 20),
        name="final_grad",
    )(*dps, dqa, dqb, projected, hidden, loss)


def x_ring(k):
    return [(j, (j // 4) * 4 + (j % 4 + k) % 4) for j in range(32)]


def z_ring(k):
    return [(j, (j // 16 * 4 + (j // 4 % 4 + k) % 4) * 4 + j % 4) for j in range(32)]


def y_swap():
    return [(j, (j + 16) % 32) for j in range(32)]


def inverse(pairs):
    return [(b, a) for a, b in pairs]


def per_device(
    query_states, passage_states, query_lengths, passage_lengths, passage_ids, positives,
    up_weight, up_bias, down_weight, down_bias, norm_gain, norm_bias, proj_weight,
):
    p_dev, p_len, _ = passage_states.shape
    queries = query_states.shape[0] * lax.axis_size("rep") * lax.axis_size("dp")
    me = lax.axis_index("dp").reshape(1)
    hidden, projected, qsend, psend = encode(
        query_states, jnp.swapaxes(passage_states, 0, 1), query_lengths, passage_lengths, passage_ids,
        positives, up_weight, up_bias, down_weight, down_bias, norm_gain, norm_bias, proj_weight,
    )
    other = lax.ppermute(qsend, "dp", y_swap())
    ps = [psend] + [lax.ppermute(psend, "dp", x_ring(k)) for k in range(1, X_PEERS)]
    pair = jnp.stack([qsend, other])
    qs = [pair] + [lax.ppermute(pair, "dp", z_ring(k)) for k in range(1, 4)]
    sc, tot, zpart, e = forward(me, qs, ps)
    za = zpart + sum(lax.ppermute(zpart, "dp", z_ring(k)) for k in range(1, 4))
    zb = lax.ppermute(za, "dp", y_swap())
    dps, dqs, loss = backward(me, qs, ps, sc, tot, za, zb, e)
    dq = dqs[0].astype(f32)
    for k in range(1, 4):
        dq = dq + lax.ppermute(dqs[k], "dp", inverse(z_ring(k))).astype(f32)
    dps = [dps[0]] + [lax.ppermute(dps[k], "dp", inverse(x_ring(k))) for k in range(1, X_PEERS)]
    dqb = lax.ppermute(dq[1].astype(bf16), "dp", y_swap())
    pgrad, share = final(dps, dq[0], dqb, projected, hidden, loss)
    passage_grad = jnp.swapaxes(pgrad.reshape(p_len, p_dev, EMB), 0, 1)
    parts = lax.all_to_all(share, ("rep", "dp"), 0, 0, tiled=True)
    summed = jnp.sum(parts.astype(f32), axis=0)
    mean_loss = (summed[6, 0] + summed[7, 0]) / queries
    out = jnp.broadcast_to(summed.astype(bf16)[None], parts.shape)
    pieces = lax.all_to_all(out, ("rep", "dp"), 0, 0, tiled=True)
    proj_grad = jnp.swapaxes(pieces[:, :6, :], 0, 1).reshape(768, 128).astype(f32)
    return (mean_loss, passage_grad, proj_grad)


def solution(mesh):
    rows = P(("rep", "dp"))
    in_specs = (rows,) * 6 + (P(),) * 7
    out_specs = (P(), rows, P())
    return jax.shard_map(
        per_device, mesh=mesh, in_specs=in_specs, out_specs=out_specs, check_vma=False
    )
```

```python
import jax
import jax.numpy as jnp
from jax import lax
from jax.experimental import pallas as pl
from jax.experimental.pallas import tpu as pltpu
from jax.sharding import PartitionSpec as P

temper = 0.05
eps_norm = 1e-06
punct_low = 999
punct_high = 1067

bf16 = jnp.bfloat16
f32 = jnp.float32
i32 = jnp.int32


X_PEERS = 4
YZ_PEERS = 8
P_ROWS = 720
Q_ROWS = 256
EMB = 128
FCHUNK = 512
ROW_TILES = [slice(0, 256), slice(256, 496), slice(496, 736), slice(736, 976)]
SHARE = 192
MASKED = 2.0
BIAS = -10000.0
SCALE = 1.4426950408889634 / temper

VM = pl.BlockSpec(memory_space=pltpu.VMEM)
SM = pl.BlockSpec(memory_space=pltpu.SMEM)


def mm(a, b):
    return jnp.dot(a, b, preferred_element_type=f32)


def fetch(which, k, w1_ref, w2_ref, w1_s, w2_s, sem):
    c = pl.ds(pl.multiple_of(k * FCHUNK, FCHUNK), FCHUNK)
    if which == 0:
        return pltpu.make_async_copy(w1_ref.at[:, c], w1_s.at[k], sem.at[0, k])
    return pltpu.make_async_copy(w2_ref.at[c, :], w2_s.at[k], sem.at[1, k])


def feed_forward(w1_ref, b1_s, w2_ref, x_s, acc_s, act_s, w1_s, w2_s, sem, finish):
    count = w1_s.shape[0]

    def up(k, slot):
        bias = b1_s[:, pl.ds(pl.multiple_of(k * FCHUNK, FCHUNK), FCHUNK)]
        val = mm(x_s[...], w1_s[k]) + bias
        act_s[slot] = (val * 0.5 * (1.0 + lax.erf(val * 0.7071067811865476))).astype(bf16)

    fetch(0, 0, w1_ref, w2_ref, w1_s, w2_s, sem).wait()
    up(0, 0)

    def step(k, carry):
        @pl.when(k + 2 < count)
        def _():
            fetch(0, k + 2, w1_ref, w2_ref, w1_s, w2_s, sem).start()
            fetch(1, k + 2, w1_ref, w2_ref, w1_s, w2_s, sem).start()

        fetch(1, k, w1_ref, w2_ref, w1_s, w2_s, sem).wait()
        fetch(0, k + 1, w1_ref, w2_ref, w1_s, w2_s, sem).wait()
        up(k + 1, (k + 1) % 2)
        acc_s[...] += mm(act_s[k % 2], w2_s[k])
        return carry

    lax.fori_loop(0, count - 1, step, 0)
    fetch(1, count - 1, w1_ref, w2_ref, w1_s, w2_s, sem).wait()
    for m, r in enumerate(ROW_TILES):
        finish(m, r, acc_s[r, :] + mm(act_s[(count - 1) % 2, r, :], w2_s[count - 1]))


def finish_rows(r, res, gain, nbias, proj_ref, hidden_ref, projected_ref):
    width = res.shape[1]
    mean = jnp.sum(res, -1, keepdims=True) * (1.0 / width)
    cen = res - mean
    var = jnp.sum(cen * cen, -1, keepdims=True) * (1.0 / width)
    hid = (cen * lax.rsqrt(var + eps_norm) * gain + nbias).astype(bf16)
    hidden_ref[r, :] = hid
    pr = mm(hid, proj_ref[...])
    projected_ref[r, :] = pr
    return pr * lax.rsqrt(jnp.sum(pr * pr, -1, keepdims=True) + eps_norm)


def encode_kernel(
    qlen_any, pos_any, plen_any, ids_any, xq_any, xp_any, w1_ref, b1_any, w2_ref, b2_any,
    gain_any, nbias_any, proj_any, hidden_any, projected_any, qsend_any, psend_any,
    x_s, acc_s, act_s, w1_s, w2_s, sem, keep_s, ids_s, small_sem,
    qlen_ref, pos_ref, plen_ref, ids_ref, xq_ref, xp_ref, b1_ref, b2_ref, gain_ref, nbias_ref, proj_ref,
    hidden_ref, projected_ref, qsend_ref, psend_ref, out_sem,
):
    sources = (xp_any, xq_any, b2_any, ids_any, plen_any, b1_any, gain_any, nbias_any, proj_any, qlen_any, pos_any)
    targets = (xp_ref, xq_ref, b2_ref, ids_ref, plen_ref, b1_ref, gain_ref, nbias_ref, proj_ref, qlen_ref, pos_ref)
    copies = [pltpu.make_async_copy(a, b, small_sem.at[i]) for i, (a, b) in enumerate(zip(sources, targets))]
    for copy in copies[:2]:
        copy.start()
    fetch(0, 0, w1_ref, w2_ref, w1_s, w2_s, sem).start()
    for copy in copies[2:]:
        copy.start()
    q_dev, q_len, width = xq_ref.shape
    p_len, p_dev, _ = xp_ref.shape
    for copy in copies:
        copy.wait()
    fetch(1, 0, w1_ref, w2_ref, w1_s, w2_s, sem).start()
    for which in range(2):
        fetch(which, 1, w1_ref, w2_ref, w1_s, w2_s, sem).start()
    b2, gain, nbias = (v[...].reshape(1, width) for v in (b2_ref, gain_ref, nbias_ref))
    x_s[0:Q_ROWS, :] = xq_ref[...].reshape(Q_ROWS, width)
    x_s[Q_ROWS:, :] = xp_ref[...].reshape(P_ROWS, width)
    acc_s[...] = x_s[...].astype(f32) + b2
    ids_s[...] = jnp.zeros_like(ids_s)
    ids_s[0:p_dev, 0:p_len] = ids_ref[...]
    ids_s[p_dev : 2 * p_dev, 0:p_len] = ids_ref[...]
    ids = ids_s[...]
    row = lax.broadcasted_iota(i32, (8, 256), 0) % p_dev
    col = lax.broadcasted_iota(i32, (8, 256), 1)
    lens = jnp.zeros((8, 256), i32)
    for p in range(p_dev):
        lens = jnp.where(row == p, plen_ref[p], lens)
    punct = jnp.logical_and(ids >= punct_low, ids < punct_high)
    keep = jnp.where(jnp.logical_and(col < lens, jnp.logical_not(punct)), 1.0, 0.0)
    ones = jnp.ones((256, EMB), bf16)
    slab = lax.broadcasted_iota(i32, (30, 8, 256), 0) * 2 + lax.broadcasted_iota(i32, (30, 8, 256), 1) // p_dev
    cols = lax.broadcasted_iota(i32, (30, 8, 256), 2)
    for m in range(3):
        pick = jnp.where(slab + m * 60 == cols, jnp.broadcast_to(keep[None], (30, 8, 256)), 0.0)
        keep_s[m * 240 : (m + 1) * 240, :] = mm(pick.reshape(240, 256).astype(bf16), ones)
    row = lax.broadcasted_iota(i32, (16, EMB), 0)
    token = lax.broadcasted_iota(i32, (16, EMB), 1) + EMB * (row % 2)
    owner = token // q_len
    slot = token % q_len
    lens = jnp.zeros((16, EMB), i32)
    posi = jnp.zeros((16, EMB), i32)
    for q in range(q_dev):
        lens = jnp.where(owner == q, qlen_ref[q], lens)
        posi = jnp.where(owner == q, pos_ref[q], posi)
    kept = jnp.where(slot < lens, 1.0, 0.0)
    meta = jnp.where(row < 2, kept, jnp.where(row < 4, posi.astype(f32), 0.0)).astype(bf16)
    qsend_ref[Q_ROWS : Q_ROWS + 16, :] = meta
    outs = []

    def put(src, dst):
        outs.append(pltpu.make_async_copy(src, dst, out_sem.at[len(outs)]))
        outs[-1].start()

    def finish(m, r, res):
        normed = finish_rows(r, res, gain, nbias, proj_ref, hidden_ref, projected_ref)
        if m == 0:
            qsend_ref[r, :] = normed.astype(bf16)
            put(qsend_ref, qsend_any)
        else:
            s = slice(r.start - Q_ROWS, r.stop - Q_ROWS)
            psend_ref[s, :] = jnp.where(keep_s[s, :] > 0.5, normed, MASKED).astype(bf16)
            put(psend_ref.at[s, :], psend_any.at[s, :])
        put(hidden_ref.at[r, :], hidden_any.at[r, :])
        put(projected_ref.at[r, :], projected_any.at[r, :])

    feed_forward(w1_ref, b1_ref, w2_ref, x_s, acc_s, act_s, w1_s, w2_s, sem, finish)
    for copy in outs:
        copy.wait()


def encode(xq, xp, qlen, plen, ids, pos, w1, b1, w2, b2, gain, nbias, proj):
    width, ff = w1.shape
    count = ff // FCHUNK
    rows = Q_ROWS + P_ROWS
    far = pl.BlockSpec(memory_space=pltpu.HBM)
    return pl.pallas_call(
        encode_kernel,
        in_specs=[far] * 13,
        out_specs=[far] * 4,
        out_shape=[
            jax.ShapeDtypeStruct((rows, width), bf16),
            jax.ShapeDtypeStruct((rows, EMB), f32),
            jax.ShapeDtypeStruct((Q_ROWS + 16, EMB), bf16),
            jax.ShapeDtypeStruct((P_ROWS, EMB), bf16),
        ],
        scratch_shapes=[
            pltpu.VMEM((rows, width), bf16),
            pltpu.VMEM((rows, width), f32),
            pltpu.VMEM((2, rows, FCHUNK), bf16),
            pltpu.VMEM((count, width, FCHUNK), bf16),
            pltpu.VMEM((count, FCHUNK, width), bf16),
            pltpu.SemaphoreType.DMA((2, count)),
            pltpu.VMEM((P_ROWS, EMB), f32),
            pltpu.VMEM((8, 256), i32),
            pltpu.SemaphoreType.DMA((11,)),
            pltpu.SMEM(qlen.shape, i32),
            pltpu.SMEM(pos.shape, i32),
            pltpu.SMEM(plen.shape, i32),
            pltpu.VMEM(ids.shape, i32),
            pltpu.VMEM(xq.shape, bf16),
            pltpu.VMEM(xp.shape, bf16),
            pltpu.VMEM((1, ff), f32),
            pltpu.VMEM((width,), f32),
            pltpu.VMEM((width,), f32),
            pltpu.VMEM((width,), f32),
            pltpu.VMEM(proj.shape, bf16),
            pltpu.VMEM((rows, width), bf16),
            pltpu.VMEM((rows, EMB), f32),
            pltpu.VMEM((Q_ROWS + 16, EMB), bf16),
            pltpu.VMEM((P_ROWS, EMB), bf16),
            pltpu.SemaphoreType.DMA((3 * len(ROW_TILES),)),
        ],
        cost_estimate=pl.CostEstimate(flops=4 * rows * width * ff, bytes_accessed=4 * width * ff, transcendentals=rows * ff),
        name="encode",
    )(qlen, pos, plen, ids, xq, xp, w1, b1[None], w2, b2, gain, nbias, proj)


def load_pairs(q_refs, p_refs, qt_s, pa_s, keep_s):
    for k in range(YZ_PEERS):
        q_ref = q_refs[k // 2]
        qt_s[0:EMB, k * 256 : (k + 1) * 256] = q_ref[k % 2, 0:Q_ROWS, :].T
        for h in range(2):
            keep_s[:, k * 256 + h * 128 : k * 256 + (h + 1) * 128] = q_ref[k % 2, 256 + h : 257 + h, :].astype(f32)
    cols = qt_s.shape[1]
    first = lax.broadcasted_iota(i32, (EMB, cols), 0) == 0
    qt_s[EMB : 2 * EMB, :] = jnp.where(first, 1.0, 0.0).astype(bf16)
    for k, p_ref in enumerate(p_refs):
        r = slice(k * P_ROWS, (k + 1) * P_ROWS)
        val = p_ref[...]
        pa_s[r, 0:EMB] = val
        pa_s[r, EMB : 2 * EMB] = jnp.where(val.astype(f32) > 1.5, BIAS, 0.0).astype(bf16)


def origin(me, block):
    yz = me // X_PEERS
    y = (yz // 4 + block % 2) % 2
    return y * 4 + (yz % 4 + 4 - block // 2) % 4


def forward_kernel(me_ref, *refs):
    q_refs, p_refs = refs[:4], refs[4 : 4 + X_PEERS]
    sc_ref, tot_ref, zpart_ref, e_ref, pt_ref, qt_s, pa_s, keep_s, sum_s = refs[4 + X_PEERS :]
    load_pairs(q_refs, p_refs, qt_s, pa_s, keep_s)
    for i in range(0, pa_s.shape[0], 128):
        n = min(128, pa_s.shape[0] - i)
        pt_ref[:, i : i + n] = pa_s[i : i + n, 0:EMB].T
    cols = qt_s.shape[1]

    def group(g, carry):
        for j in range(cols // 256):
            c = slice(j * 256, (j + 1) * 256)
            total = jnp.zeros((8, 256), f32)
            for m in range(3):
                r = pl.ds(pl.multiple_of(g * P_ROWS + m * 240, 16), 240)
                e = jnp.exp2(mm(pa_s[r, :], qt_s[:, c]) * SCALE)
                e_ref[r, c] = e.astype(bf16)
                total = total + jnp.sum(e.reshape(30, 8, 256), axis=0)
            sum_s[pl.ds(pl.multiple_of(g * 8, 8), 8), c] = total
        return carry

    lax.fori_loop(0, X_PEERS, group, 0)
    for g in range(X_PEERS):
        tot_ref[4 * g : 4 * g + 4, :] = sum_s[8 * g : 8 * g + 4, :] + sum_s[8 * g + 4 : 8 * g + 8, :]
    a = lax.broadcasted_iota(i32, (128, 128), 0) // 32
    b = lax.broadcasted_iota(i32, (128, 128), 1) // 32
    same = jnp.where(a == b, 1.0, 0.0)
    for t in range(cols // 128):
        c = slice(t * 128, (t + 1) * 128)
        soft = jnp.log(tot_ref[:, c]) * temper * keep_s[:, c]
        sc = jnp.dot(soft, same, preferred_element_type=f32, precision=lax.Precision.HIGHEST)
        sc_ref[:, c] = sc
        z = jnp.sum(jnp.exp(sc), axis=0, keepdims=True)
        zpart_ref[pl.ds(origin(me_ref[0], t // 2) * 2 + t % 2, 1), :] = z


def forward(me, qs, ps):
    cols = YZ_PEERS * Q_ROWS
    return pl.pallas_call(
        forward_kernel,
        in_specs=[SM] + [VM] * (4 + X_PEERS),
        out_specs=[VM] * 5,
        out_shape=[
            jax.ShapeDtypeStruct((16, cols), f32),
            jax.ShapeDtypeStruct((16, cols), f32),
            jax.ShapeDtypeStruct((16, 128), f32),
            jax.ShapeDtypeStruct((X_PEERS * P_ROWS, cols), bf16),
            jax.ShapeDtypeStruct((EMB, X_PEERS * P_ROWS), bf16),
        ],
        scratch_shapes=[
            pltpu.VMEM((256, cols), bf16),
            pltpu.VMEM((X_PEERS * P_ROWS, 256), bf16),
            pltpu.VMEM((1, cols), f32),
            pltpu.VMEM((8 * X_PEERS, cols), f32),
        ],
        compiler_params=pltpu.CompilerParams(vmem_limit_bytes=16 << 20),
        name="pair_forward",
    )(me, *qs, *ps)


def backward_kernel(me_ref, *refs):
    q_refs, refs = refs[:4], refs[4:]
    pt_ref, sc_ref, tot_ref, za_ref, zb_ref, e_ref = refs[:6]
    dp_refs, dq_refs, refs = refs[6 : 6 + X_PEERS], refs[6 + X_PEERS : 10 + X_PEERS], refs[10 + X_PEERS :]
    loss_ref, q_s, fac_s, g_s, dp_s = refs
    p_all, cols = g_s.shape
    for k in range(YZ_PEERS):
        q_s[k * 256 : (k + 1) * 256, :] = q_refs[k // 2][k % 2, 0:Q_ROWS, :]
    me = me_ref[0]
    x = me % X_PEERS
    row = lax.broadcasted_iota(i32, (16, 128), 0)
    number = row % 4 + (me // X_PEERS) * 16
    for k in range(X_PEERS):
        number = jnp.where(row // 4 == k, number + ((x + X_PEERS - k) % X_PEERS) * 4, number)
    number = number.astype(f32)
    lane = lax.broadcasted_iota(i32, (1, 128), 1)
    head = jnp.where(lane % 32 == 0, 1.0, 0.0)
    loss = jnp.zeros((1, 128), f32)
    for t in range(cols // 128):
        c = slice(t * 128, (t + 1) * 128)
        at = pl.ds(origin(me, t // 2) * 2 + t % 2, 1)
        z = za_ref[at, :] + zb_ref[at, :]
        sc = sc_ref[:, c]
        q_ref, a = q_refs[t // 4], t // 2 % 2
        keep = q_ref[a, 256 + t % 2 : 257 + t % 2, :].astype(f32)
        pos = q_ref[a, 258 + t % 2 : 259 + t % 2, :].astype(f32)
        hit = jnp.where(number == pos, 1.0, 0.0)
        fac = (jnp.exp(sc) / z - hit) * (keep / tot_ref[:, c])
        for g in range(X_PEERS):
            fac_s[8 * g : 8 * g + 4, c] = fac[4 * g : 4 * g + 4, :]
            fac_s[8 * g + 4 : 8 * g + 8, c] = fac[4 * g : 4 * g + 4, :]
        loss = loss + (jnp.log(z) * (1.0 / YZ_PEERS) - jnp.sum(hit * sc, axis=0, keepdims=True)) * head
    loss_ref[...] = jnp.broadcast_to(jnp.sum(loss, axis=1, keepdims=True), loss_ref.shape)

    def group(g, carry):
        for m in range(3):
            r = pl.ds(pl.multiple_of(g * P_ROWS + m * 240, 16), 240)
            for j in range(cols // 256):
                c = slice(j * 256, (j + 1) * 256)
                fac = fac_s[pl.ds(pl.multiple_of(g * 8, 8), 8), c]
                grad = e_ref[r, c].astype(f32).reshape(30, 8, 256) * fac[None]
                g_s[r, c] = grad.reshape(240, 256).astype(bf16)
            dp_s[r, :] = mm(g_s[r, :], q_s[...])
        return carry

    lax.fori_loop(0, X_PEERS, group, 0)

    for k in range(4):
        dq = mm(pt_ref[...], g_s[:, k * 512 : (k + 1) * 512]).astype(bf16)
        for h in range(2):
            dq_refs[k][h] = dq[:, h * 256 : (h + 1) * 256]
    for k in range(X_PEERS):
        dp_refs[k][...] = dp_s[k * P_ROWS : (k + 1) * P_ROWS, :].astype(dp_refs[k].dtype)


def backward(me, qs, pt, sc, tot, za, zb, e):
    p_all, cols = e.shape
    out = pl.pallas_call(
        backward_kernel,
        in_specs=[SM] + [VM] * 10,
        out_specs=[VM] * (X_PEERS + 5),
        out_shape=[jax.ShapeDtypeStruct((P_ROWS, EMB), f32 if k == 0 else bf16) for k in range(X_PEERS)]
        + [jax.ShapeDtypeStruct((2, EMB, Q_ROWS), bf16)] * 4
        + [jax.ShapeDtypeStruct((1, 128), f32)],
        scratch_shapes=[
            pltpu.VMEM((cols, EMB), bf16),
            pltpu.VMEM((8 * X_PEERS, cols), f32),
            pltpu.VMEM((p_all, cols), bf16),
            pltpu.VMEM((p_all, EMB), f32),
        ],
        compiler_params=pltpu.CompilerParams(vmem_limit_bytes=24 << 20),
        name="pair_backward",
    )(me, *qs, pt, sc, tot, za, zb, e)
    return out[:X_PEERS], out[X_PEERS : X_PEERS + 4], out[-1]


def with_loss(loss):
    row = lax.broadcasted_iota(i32, (8, EMB), 0)
    high = loss.astype(bf16).astype(f32)
    return jnp.where(row == 0, high, jnp.where(row == 1, loss - high, 0.0)).astype(bf16)


def final_kernel(me_ref, *refs):
    dp_refs, refs = refs[:X_PEERS], refs[X_PEERS:]
    dqa_ref, dqb_ref, projected_ref, hidden_ref, loss_ref, pgrad_ref = refs[:6]
    share_refs = refs[6 : 6 + X_PEERS]
    bt_s, bp_s, share_s = refs[6 + X_PEERS :]
    pr = projected_ref[0:Q_ROWS, :]
    inv = lax.rsqrt(jnp.sum(pr * pr, -1, keepdims=True) + eps_norm)
    nt = (pr * inv).T
    it = jnp.broadcast_to(inv, pr.shape).T
    grad = dqa_ref[...] + dqb_ref[...].astype(f32)
    dot = jnp.sum(nt * grad, axis=0, keepdims=True)
    bt_s[...] = (it * (grad - nt * dot)).astype(bf16)
    for m in range(3):
        r = slice(m * 240, (m + 1) * 240)
        grad = dp_refs[0][r, :].astype(f32)
        for k in range(1, X_PEERS):
            grad = grad + dp_refs[k][r, :].astype(f32)
        pgrad_ref[r, :] = grad
        pr = projected_ref[Q_ROWS + m * 240 : Q_ROWS + (m + 1) * 240, :]
        inv = lax.rsqrt(jnp.sum(pr * pr, -1, keepdims=True) + eps_norm)
        nm = pr * inv
        bp_s[r, :] = inv * (grad - nm * jnp.sum(nm * grad, -1, keepdims=True))
    bpt = bp_s[...].T.astype(bf16)
    for k in range(6):
        c = slice(k * 128, (k + 1) * 128)
        pg = mm(bt_s[...], hidden_ref[0:Q_ROWS, c]) + mm(bpt, hidden_ref[Q_ROWS:, c])
        share_s[c, :] = pg.T
    tail = with_loss(loss_ref[...])
    for k in range(X_PEERS):
        block = (me_ref[0] + k) % X_PEERS
        share_refs[k][0:SHARE, :] = share_s[pl.ds(pl.multiple_of(block * SHARE, SHARE), SHARE), :].astype(bf16)
        share_refs[k][SHARE:, :] = tail


def final(me, dps, dqa, dqb, projected, hidden, loss):
    return pl.pallas_call(
        final_kernel,
        in_specs=[SM] + [VM] * (X_PEERS + 5),
        out_specs=[VM] * (X_PEERS + 1),
        out_shape=[jax.ShapeDtypeStruct((P_ROWS, EMB), f32)]
        + [jax.ShapeDtypeStruct((SHARE + 8, EMB), bf16)] * X_PEERS,
        scratch_shapes=[
            pltpu.VMEM((EMB, Q_ROWS), bf16),
            pltpu.VMEM((P_ROWS, EMB), f32),
            pltpu.VMEM((X_PEERS * SHARE, EMB), f32),
        ],
        compiler_params=pltpu.CompilerParams(vmem_limit_bytes=12 << 20),
        name="final_grad",
    )(me, *dps, dqa, dqb, projected, hidden, loss)


def combine_kernel(*refs):
    *ins, out_ref = refs
    vals = [r[...].astype(f32) for r in ins]
    total = vals[0] + vals[1] if len(vals) == 2 else (vals[0] + vals[2]) + (vals[1] + vals[3])
    out_ref[0:SHARE, :] = total[0:SHARE].astype(bf16)
    out_ref[SHARE:, :] = with_loss(total[SHARE : SHARE + 1] + total[SHARE + 1 : SHARE + 2])


def combine(parts):
    return pl.pallas_call(
        combine_kernel,
        in_specs=[VM] * len(parts),
        out_specs=VM,
        out_shape=jax.ShapeDtypeStruct((SHARE + 8, EMB), bf16),
        compiler_params=pltpu.CompilerParams(vmem_limit_bytes=4 << 20),
        name="combine",
    )(*parts)


def assemble_kernel(me_ref, *refs):
    *ins, out_ref = refs
    for k in range(X_PEERS):
        block = (me_ref[0] + X_PEERS - k) % X_PEERS
        out_ref[pl.ds(pl.multiple_of(block * SHARE, SHARE), SHARE), :] = ins[k][0:SHARE, :].astype(f32)


def assemble(me, parts):
    return pl.pallas_call(
        assemble_kernel,
        in_specs=[SM] + [VM] * len(parts),
        out_specs=VM,
        out_shape=jax.ShapeDtypeStruct((X_PEERS * SHARE, EMB), f32),
        compiler_params=pltpu.CompilerParams(vmem_limit_bytes=4 << 20),
        name="assemble",
    )(me, *parts)


def x_ring(k):
    return [(j, (j // 4) * 4 + (j % 4 + k) % 4) for j in range(32)]


def z_ring(k):
    return [(j, (j // 16 * 4 + (j // 4 % 4 + k) % 4) * 4 + j % 4) for j in range(32)]


def y_swap():
    return [(j, (j + 16) % 32) for j in range(32)]


def y_ring(k):
    def to(j):
        rep, dp = j // 32, j % 32
        y = (rep // 2 * 2 + dp // 16 + k) % 4
        return (y // 2 * 2 + rep % 2) * 32 + y % 2 * 16 + dp % 16

    return [(j, to(j)) for j in range(128)]


def inverse(pairs):
    return [(b, a) for a, b in pairs]


def per_device(
    query_states, passage_states, query_lengths, passage_lengths, passage_ids, positives,
    up_weight, up_bias, down_weight, down_bias, norm_gain, norm_bias, proj_weight,
):
    p_dev, p_len, _ = passage_states.shape
    queries = query_states.shape[0] * lax.axis_size("rep") * lax.axis_size("dp")
    me = lax.axis_index("dp").reshape(1)
    hidden, projected, qsend, psend = encode(
        query_states, jnp.swapaxes(passage_states, 0, 1), query_lengths, passage_lengths, passage_ids,
        positives, up_weight, up_bias, down_weight, down_bias, norm_gain, norm_bias, proj_weight,
    )
    other = lax.ppermute(qsend, "dp", y_swap())
    ps = [psend] + [lax.ppermute(psend, "dp", x_ring(k)) for k in range(1, X_PEERS)]
    pair = jnp.stack([qsend, other])
    qs = [pair] + [lax.ppermute(pair, "dp", z_ring(k)) for k in range(1, 4)]
    sc, tot, zpart, e, pt = forward(me, qs, ps)
    za = zpart + sum(lax.ppermute(zpart, "dp", z_ring(k)) for k in range(1, 4))
    zb = lax.ppermute(za, "dp", y_swap())
    dps, dqs, loss = backward(me, qs, pt, sc, tot, za, zb, e)
    dq = dqs[0].astype(f32)
    for k in range(1, 4):
        dq = dq + lax.ppermute(dqs[k], "dp", inverse(z_ring(k))).astype(f32)
    dps = [dps[0]] + [lax.ppermute(dps[k], "dp", inverse(x_ring(k))) for k in range(1, X_PEERS)]
    dqb = lax.ppermute(dq[1].astype(bf16), "dp", y_swap())
    pgrad, *shares = final(me, dps, dq[0], dqb, projected, hidden, loss)
    passage_grad = jnp.swapaxes(pgrad.reshape(p_len, p_dev, EMB), 0, 1)
    part = combine([shares[0]] + [lax.ppermute(shares[k], "dp", x_ring(k)) for k in range(1, X_PEERS)])
    part = combine([part] + [lax.ppermute(part, "dp", z_ring(k)) for k in range(1, 4)])
    part = combine([part] + [lax.ppermute(part, ("rep", "dp"), y_ring(k)) for k in range(1, 4)])
    part = combine([part, lax.ppermute(part, "rep", [(0, 1), (1, 0), (2, 3), (3, 2)])])
    mean_loss = (part[SHARE, 0].astype(f32) + part[SHARE + 1, 0].astype(f32)) / queries
    proj_grad = assemble(me, [part] + [lax.ppermute(part, "dp", x_ring(k)) for k in range(1, X_PEERS)])
    return (mean_loss, passage_grad, proj_grad)


def solution(mesh):
    rows = P(("rep", "dp"))
    in_specs = (rows,) * 6 + (P(),) * 7
    out_specs = (P(), rows, P())
    return jax.shard_map(
        per_device, mesh=mesh, in_specs=in_specs, out_specs=out_specs, check_vma=False
    )
```

```python
import jax
import jax.numpy as jnp
from jax import lax
from jax.experimental import pallas as pl
from jax.experimental.pallas import tpu as pltpu
from jax.sharding import PartitionSpec as P

temper = 0.05
eps_norm = 1e-06
punct_low = 999
punct_high = 1067

bf16 = jnp.bfloat16
f32 = jnp.float32
i32 = jnp.int32


X_PEERS = 4
YZ_PEERS = 8
P_ROWS = 720
Q_ROWS = 256
EMB = 128
FCHUNK = 512
ROW_TILES = [slice(0, 256), slice(256, 496), slice(496, 736), slice(736, 976)]
SHARE = 384
CORES = 2
MASKED = 2.0
BIAS = -10000.0
SCALE = 1.4426950408889634 / temper

VM = pl.BlockSpec(memory_space=pltpu.VMEM)
SM = pl.BlockSpec(memory_space=pltpu.SMEM)


def mm(a, b):
    return jnp.dot(a, b, preferred_element_type=f32)


def fetch(which, k, w1_ref, w2_ref, w1_s, w2_s, sem):
    c = pl.ds(pl.multiple_of(k * FCHUNK, FCHUNK), FCHUNK)
    if which == 0:
        return pltpu.make_async_copy(w1_ref.at[:, c], w1_s.at[k], sem.at[0, k])
    return pltpu.make_async_copy(w2_ref.at[c, :], w2_s.at[k], sem.at[1, k])


def feed_forward(w1_ref, b1_s, w2_ref, x_s, acc_s, act_s, w1_s, w2_s, sem, finish):
    count = w1_s.shape[0]

    def up(k, slot):
        bias = b1_s[:, pl.ds(pl.multiple_of(k * FCHUNK, FCHUNK), FCHUNK)]
        val = mm(x_s[...], w1_s[k]) + bias
        act_s[slot] = (val * 0.5 * (1.0 + lax.erf(val * 0.7071067811865476))).astype(bf16)

    fetch(0, 0, w1_ref, w2_ref, w1_s, w2_s, sem).wait()
    up(0, 0)

    def step(k, carry):
        @pl.when(k + 2 < count)
        def _():
            fetch(0, k + 2, w1_ref, w2_ref, w1_s, w2_s, sem).start()
            fetch(1, k + 2, w1_ref, w2_ref, w1_s, w2_s, sem).start()

        fetch(1, k, w1_ref, w2_ref, w1_s, w2_s, sem).wait()
        fetch(0, k + 1, w1_ref, w2_ref, w1_s, w2_s, sem).wait()
        up(k + 1, (k + 1) % 2)
        acc_s[...] += mm(act_s[k % 2], w2_s[k])
        return carry

    lax.fori_loop(0, count - 1, step, 0)
    fetch(1, count - 1, w1_ref, w2_ref, w1_s, w2_s, sem).wait()
    for m, r in enumerate(ROW_TILES):
        finish(m, r, acc_s[r, :] + mm(act_s[(count - 1) % 2, r, :], w2_s[count - 1]))


def finish_rows(r, res, gain, nbias, proj_ref, hidden_ref, projected_ref):
    width = res.shape[1]
    mean = jnp.sum(res, -1, keepdims=True) * (1.0 / width)
    cen = res - mean
    var = jnp.sum(cen * cen, -1, keepdims=True) * (1.0 / width)
    hid = (cen * lax.rsqrt(var + eps_norm) * gain + nbias).astype(bf16)
    hidden_ref[r, :] = hid
    pr = mm(hid, proj_ref[...])
    projected_ref[r, :] = pr
    return pr * lax.rsqrt(jnp.sum(pr * pr, -1, keepdims=True) + eps_norm)


def encode_kernel(
    qlen_any, pos_any, plen_any, ids_any, xq_any, xp_any, w1_ref, b1_any, w2_ref, b2_any,
    gain_any, nbias_any, proj_any, hidden_any, projected_any, qsend_any, psend_any,
    x_s, acc_s, act_s, w1_s, w2_s, sem, keep_s, ids_s, small_sem,
    qlen_ref, pos_ref, plen_ref, ids_ref, xq_ref, xp_ref, b1_ref, b2_ref, gain_ref, nbias_ref, proj_ref,
    hidden_ref, projected_ref, qsend_ref, psend_ref, out_sem,
):
    sources = (xp_any, xq_any, b2_any, ids_any, plen_any, b1_any, gain_any, nbias_any, proj_any, qlen_any, pos_any)
    targets = (xp_ref, xq_ref, b2_ref, ids_ref, plen_ref, b1_ref, gain_ref, nbias_ref, proj_ref, qlen_ref, pos_ref)
    copies = [pltpu.make_async_copy(a, b, small_sem.at[i]) for i, (a, b) in enumerate(zip(sources, targets))]
    for copy in copies[:2]:
        copy.start()
    fetch(0, 0, w1_ref, w2_ref, w1_s, w2_s, sem).start()
    for copy in copies[2:]:
        copy.start()
    q_dev, q_len, width = xq_ref.shape
    p_len, p_dev, _ = xp_ref.shape
    for copy in copies:
        copy.wait()
    fetch(1, 0, w1_ref, w2_ref, w1_s, w2_s, sem).start()
    for which in range(2):
        fetch(which, 1, w1_ref, w2_ref, w1_s, w2_s, sem).start()
    b2, gain, nbias = (v[...].reshape(1, width) for v in (b2_ref, gain_ref, nbias_ref))
    x_s[0:Q_ROWS, :] = xq_ref[...].reshape(Q_ROWS, width)
    x_s[Q_ROWS:, :] = xp_ref[...].reshape(P_ROWS, width)
    acc_s[...] = x_s[...].astype(f32) + b2
    ids_s[...] = jnp.zeros_like(ids_s)
    ids_s[0:p_dev, 0:p_len] = ids_ref[...]
    ids_s[p_dev : 2 * p_dev, 0:p_len] = ids_ref[...]
    ids = ids_s[...]
    row = lax.broadcasted_iota(i32, (8, 256), 0) % p_dev
    col = lax.broadcasted_iota(i32, (8, 256), 1)
    lens = jnp.zeros((8, 256), i32)
    for p in range(p_dev):
        lens = jnp.where(row == p, plen_ref[p], lens)
    punct = jnp.logical_and(ids >= punct_low, ids < punct_high)
    keep = jnp.where(jnp.logical_and(col < lens, jnp.logical_not(punct)), 1.0, 0.0)
    ones = jnp.ones((256, EMB), bf16)
    slab = lax.broadcasted_iota(i32, (30, 8, 256), 0) * 2 + lax.broadcasted_iota(i32, (30, 8, 256), 1) // p_dev
    cols = lax.broadcasted_iota(i32, (30, 8, 256), 2)
    for m in range(3):
        pick = jnp.where(slab + m * 60 == cols, jnp.broadcast_to(keep[None], (30, 8, 256)), 0.0)
        keep_s[m * 240 : (m + 1) * 240, :] = mm(pick.reshape(240, 256).astype(bf16), ones)
    row = lax.broadcasted_iota(i32, (16, EMB), 0)
    token = lax.broadcasted_iota(i32, (16, EMB), 1) + EMB * (row % 2)
    owner = token // q_len
    slot = token % q_len
    lens = jnp.zeros((16, EMB), i32)
    posi = jnp.zeros((16, EMB), i32)
    for q in range(q_dev):
        lens = jnp.where(owner == q, qlen_ref[q], lens)
        posi = jnp.where(owner == q, pos_ref[q], posi)
    kept = jnp.where(slot < lens, 1.0, 0.0)
    meta = jnp.where(row < 2, kept, jnp.where(row < 4, posi.astype(f32), 0.0)).astype(bf16)
    qsend_ref[Q_ROWS : Q_ROWS + 16, :] = meta
    outs = []

    def put(src, dst):
        outs.append(pltpu.make_async_copy(src, dst, out_sem.at[len(outs)]))
        outs[-1].start()

    def finish(m, r, res):
        normed = finish_rows(r, res, gain, nbias, proj_ref, hidden_ref, projected_ref)
        if m == 0:
            qsend_ref[r, :] = normed.astype(bf16)
            put(qsend_ref, qsend_any)
        else:
            s = slice(r.start - Q_ROWS, r.stop - Q_ROWS)
            psend_ref[s, :] = jnp.where(keep_s[s, :] > 0.5, normed, MASKED).astype(bf16)
            put(psend_ref.at[s, :], psend_any.at[s, :])
        put(hidden_ref.at[r, :], hidden_any.at[r, :])
        put(projected_ref.at[r, :], projected_any.at[r, :])

    feed_forward(w1_ref, b1_ref, w2_ref, x_s, acc_s, act_s, w1_s, w2_s, sem, finish)
    for copy in outs:
        copy.wait()


def encode(xq, xp, qlen, plen, ids, pos, w1, b1, w2, b2, gain, nbias, proj):
    width, ff = w1.shape
    count = ff // FCHUNK
    rows = Q_ROWS + P_ROWS
    far = pl.BlockSpec(memory_space=pltpu.HBM)
    return pl.pallas_call(
        encode_kernel,
        in_specs=[far] * 13,
        out_specs=[far] * 4,
        out_shape=[
            jax.ShapeDtypeStruct((rows, width), bf16),
            jax.ShapeDtypeStruct((rows, EMB), f32),
            jax.ShapeDtypeStruct((Q_ROWS + 16, EMB), bf16),
            jax.ShapeDtypeStruct((P_ROWS, EMB), bf16),
        ],
        scratch_shapes=[
            pltpu.VMEM((rows, width), bf16),
            pltpu.VMEM((rows, width), f32),
            pltpu.VMEM((2, rows, FCHUNK), bf16),
            pltpu.VMEM((count, width, FCHUNK), bf16),
            pltpu.VMEM((count, FCHUNK, width), bf16),
            pltpu.SemaphoreType.DMA((2, count)),
            pltpu.VMEM((P_ROWS, EMB), f32),
            pltpu.VMEM((8, 256), i32),
            pltpu.SemaphoreType.DMA((11,)),
            pltpu.SMEM(qlen.shape, i32),
            pltpu.SMEM(pos.shape, i32),
            pltpu.SMEM(plen.shape, i32),
            pltpu.VMEM(ids.shape, i32),
            pltpu.VMEM(xq.shape, bf16),
            pltpu.VMEM(xp.shape, bf16),
            pltpu.VMEM((1, ff), f32),
            pltpu.VMEM((width,), f32),
            pltpu.VMEM((width,), f32),
            pltpu.VMEM((width,), f32),
            pltpu.VMEM(proj.shape, bf16),
            pltpu.VMEM((rows, width), bf16),
            pltpu.VMEM((rows, EMB), f32),
            pltpu.VMEM((Q_ROWS + 16, EMB), bf16),
            pltpu.VMEM((P_ROWS, EMB), bf16),
            pltpu.SemaphoreType.DMA((3 * len(ROW_TILES),)),
        ],
        cost_estimate=pl.CostEstimate(flops=4 * rows * width * ff, bytes_accessed=4 * width * ff, transcendentals=rows * ff),
        name="encode",
    )(qlen, pos, plen, ids, xq, xp, w1, b1[None], w2, b2, gain, nbias, proj)


def load_pairs(q_refs, p_refs, qt_s, pa_s, keep_s):
    for k in range(YZ_PEERS):
        q_ref = q_refs[k // 2]
        qt_s[0:EMB, k * 256 : (k + 1) * 256] = q_ref[k % 2, 0:Q_ROWS, :].T
        for h in range(2):
            keep_s[:, k * 256 + h * 128 : k * 256 + (h + 1) * 128] = q_ref[k % 2, 256 + h : 257 + h, :].astype(f32)
    cols = qt_s.shape[1]
    first = lax.broadcasted_iota(i32, (EMB, cols), 0) == 0
    qt_s[EMB : 2 * EMB, :] = jnp.where(first, 1.0, 0.0).astype(bf16)
    for k, p_ref in enumerate(p_refs):
        r = slice(k * P_ROWS, (k + 1) * P_ROWS)
        val = p_ref[...]
        pa_s[r, 0:EMB] = val
        pa_s[r, EMB : 2 * EMB] = jnp.where(val.astype(f32) > 1.5, BIAS, 0.0).astype(bf16)


def origin(me, block):
    yz = me // X_PEERS
    y = (yz // 4 + block % 2) % 2
    return y * 4 + (yz % 4 + 4 - block // 2) % 4


def forward_kernel(me_ref, *refs):
    q_refs, p_refs = refs[:4], refs[4 : 4 + X_PEERS]
    sc_ref, tot_ref, zpart_ref, e_ref, pt_ref, qt_s, pa_s, keep_s, sum_s = refs[4 + X_PEERS :]
    load_pairs(q_refs, p_refs, qt_s, pa_s, keep_s)
    for i in range(0, pa_s.shape[0], 128):
        n = min(128, pa_s.shape[0] - i)
        pt_ref[:, i : i + n] = pa_s[i : i + n, 0:EMB].T
    cols = qt_s.shape[1]

    def group(g, carry):
        for j in range(cols // 256):
            c = slice(j * 256, (j + 1) * 256)
            total = jnp.zeros((8, 256), f32)
            for m in range(3):
                r = pl.ds(pl.multiple_of(g * P_ROWS + m * 240, 16), 240)
                e = jnp.exp2(mm(pa_s[r, :], qt_s[:, c]) * SCALE)
                e_ref[r, c] = e.astype(bf16)
                total = total + jnp.sum(e.reshape(30, 8, 256), axis=0)
            sum_s[pl.ds(pl.multiple_of(g * 8, 8), 8), c] = total
        return carry

    lax.fori_loop(0, X_PEERS, group, 0)
    for g in range(X_PEERS):
        tot_ref[4 * g : 4 * g + 4, :] = sum_s[8 * g : 8 * g + 4, :] + sum_s[8 * g + 4 : 8 * g + 8, :]
    a = lax.broadcasted_iota(i32, (128, 128), 0) // 32
    b = lax.broadcasted_iota(i32, (128, 128), 1) // 32
    same = jnp.where(a == b, 1.0, 0.0)
    for t in range(cols // 128):
        c = slice(t * 128, (t + 1) * 128)
        soft = jnp.log(tot_ref[:, c]) * temper * keep_s[:, c]
        sc = jnp.dot(soft, same, preferred_element_type=f32, precision=lax.Precision.HIGHEST)
        sc_ref[:, c] = sc
        z = jnp.sum(jnp.exp(sc), axis=0, keepdims=True)
        zpart_ref[pl.ds(origin(me_ref[0], t // 2) * 2 + t % 2, 1), :] = z


def forward(me, qs, ps):
    cols = YZ_PEERS * Q_ROWS
    return pl.pallas_call(
        forward_kernel,
        in_specs=[SM] + [VM] * (4 + X_PEERS),
        out_specs=[VM] * 5,
        out_shape=[
            jax.ShapeDtypeStruct((16, cols), f32),
            jax.ShapeDtypeStruct((16, cols), f32),
            jax.ShapeDtypeStruct((16, 128), f32),
            jax.ShapeDtypeStruct((X_PEERS * P_ROWS, cols), bf16),
            jax.ShapeDtypeStruct((EMB, X_PEERS * P_ROWS), bf16),
        ],
        scratch_shapes=[
            pltpu.VMEM((256, cols), bf16),
            pltpu.VMEM((X_PEERS * P_ROWS, 256), bf16),
            pltpu.VMEM((1, cols), f32),
            pltpu.VMEM((8 * X_PEERS, cols), f32),
        ],
        compiler_params=pltpu.CompilerParams(vmem_limit_bytes=16 << 20),
        name="pair_forward",
    )(me, *qs, *ps)


def backward_kernel(me_ref, *refs):
    q_refs, refs = refs[:4], refs[4:]
    pt_ref, sc_ref, tot_ref, za_ref, zb_ref, e_ref = refs[:6]
    dp_refs, dq_refs, refs = refs[6 : 6 + X_PEERS], refs[6 + X_PEERS : 10 + X_PEERS], refs[10 + X_PEERS :]
    loss_ref, q_s, fac_s, g_s, dp_s = refs
    p_all, cols = g_s.shape
    for k in range(YZ_PEERS):
        q_s[k * 256 : (k + 1) * 256, :] = q_refs[k // 2][k % 2, 0:Q_ROWS, :]
    me = me_ref[0]
    x = me % X_PEERS
    row = lax.broadcasted_iota(i32, (16, 128), 0)
    number = row % 4 + (me // X_PEERS) * 16
    for k in range(X_PEERS):
        number = jnp.where(row // 4 == k, number + ((x + X_PEERS - k) % X_PEERS) * 4, number)
    number = number.astype(f32)
    lane = lax.broadcasted_iota(i32, (1, 128), 1)
    head = jnp.where(lane % 32 == 0, 1.0, 0.0)
    loss = jnp.zeros((1, 128), f32)
    for t in range(cols // 128):
        c = slice(t * 128, (t + 1) * 128)
        at = pl.ds(origin(me, t // 2) * 2 + t % 2, 1)
        z = za_ref[at, :] + zb_ref[at, :]
        sc = sc_ref[:, c]
        q_ref, a = q_refs[t // 4], t // 2 % 2
        keep = q_ref[a, 256 + t % 2 : 257 + t % 2, :].astype(f32)
        pos = q_ref[a, 258 + t % 2 : 259 + t % 2, :].astype(f32)
        hit = jnp.where(number == pos, 1.0, 0.0)
        fac = (jnp.exp(sc) / z - hit) * (keep / tot_ref[:, c])
        for g in range(X_PEERS):
            fac_s[8 * g : 8 * g + 4, c] = fac[4 * g : 4 * g + 4, :]
            fac_s[8 * g + 4 : 8 * g + 8, c] = fac[4 * g : 4 * g + 4, :]
        loss = loss + (jnp.log(z) * (1.0 / YZ_PEERS) - jnp.sum(hit * sc, axis=0, keepdims=True)) * head
    loss_ref[...] = jnp.broadcast_to(jnp.sum(loss, axis=1, keepdims=True), loss_ref.shape)

    def group(g, carry):
        for m in range(3):
            r = pl.ds(pl.multiple_of(g * P_ROWS + m * 240, 16), 240)
            for j in range(cols // 256):
                c = slice(j * 256, (j + 1) * 256)
                fac = fac_s[pl.ds(pl.multiple_of(g * 8, 8), 8), c]
                grad = e_ref[r, c].astype(f32).reshape(30, 8, 256) * fac[None]
                g_s[r, c] = grad.reshape(240, 256).astype(bf16)
            dp_s[r, :] = mm(g_s[r, :], q_s[...])
        return carry

    lax.fori_loop(0, X_PEERS, group, 0)

    for k in range(4):
        dq = mm(pt_ref[...], g_s[:, k * 512 : (k + 1) * 512]).astype(bf16)
        for h in range(2):
            dq_refs[k][h] = dq[:, h * 256 : (h + 1) * 256]
    for k in range(X_PEERS):
        dp_refs[k][...] = dp_s[k * P_ROWS : (k + 1) * P_ROWS, :].astype(dp_refs[k].dtype)


def backward(me, qs, pt, sc, tot, za, zb, e):
    p_all, cols = e.shape
    out = pl.pallas_call(
        backward_kernel,
        in_specs=[SM] + [VM] * 10,
        out_specs=[VM] * (X_PEERS + 5),
        out_shape=[jax.ShapeDtypeStruct((P_ROWS, EMB), f32 if k == 0 else bf16) for k in range(X_PEERS)]
        + [jax.ShapeDtypeStruct((2, EMB, Q_ROWS), bf16)] * 4
        + [jax.ShapeDtypeStruct((1, 128), f32)],
        scratch_shapes=[
            pltpu.VMEM((cols, EMB), bf16),
            pltpu.VMEM((8 * X_PEERS, cols), f32),
            pltpu.VMEM((p_all, cols), bf16),
            pltpu.VMEM((p_all, EMB), f32),
        ],
        compiler_params=pltpu.CompilerParams(vmem_limit_bytes=24 << 20),
        name="pair_backward",
    )(me, *qs, pt, sc, tot, za, zb, e)
    return out[:X_PEERS], out[X_PEERS : X_PEERS + 4], out[-1]


def with_loss(loss):
    row = lax.broadcasted_iota(i32, (8, EMB), 0)
    high = loss.astype(bf16).astype(f32)
    return jnp.where(row == 0, high, jnp.where(row == 1, loss - high, 0.0)).astype(bf16)


def final_kernel(core_ref, *refs):
    dp_refs, refs = refs[:X_PEERS], refs[X_PEERS:]
    dqa_ref, dqb_ref, projected_ref, hidden_ref, loss_ref, pgrad_ref = refs[:6]
    share_refs = refs[6 : 6 + CORES]
    bt_s, bp_s, share_s = refs[6 + CORES :]
    pr = projected_ref[0:Q_ROWS, :]
    inv = lax.rsqrt(jnp.sum(pr * pr, -1, keepdims=True) + eps_norm)
    nt = (pr * inv).T
    it = jnp.broadcast_to(inv, pr.shape).T
    grad = dqa_ref[...] + dqb_ref[...].astype(f32)
    dot = jnp.sum(nt * grad, axis=0, keepdims=True)
    bt_s[...] = (it * (grad - nt * dot)).astype(bf16)
    for m in range(3):
        r = slice(m * 240, (m + 1) * 240)
        grad = dp_refs[0][r, :].astype(f32)
        for k in range(1, X_PEERS):
            grad = grad + dp_refs[k][r, :].astype(f32)
        pgrad_ref[r, :] = grad
        pr = projected_ref[Q_ROWS + m * 240 : Q_ROWS + (m + 1) * 240, :]
        inv = lax.rsqrt(jnp.sum(pr * pr, -1, keepdims=True) + eps_norm)
        nm = pr * inv
        bp_s[r, :] = inv * (grad - nm * jnp.sum(nm * grad, -1, keepdims=True))
    bpt = bp_s[...].T.astype(bf16)
    for k in range(6):
        c = slice(k * 128, (k + 1) * 128)
        pg = mm(bt_s[...], hidden_ref[0:Q_ROWS, c]) + mm(bpt, hidden_ref[Q_ROWS:, c])
        share_s[c, :] = pg.T
    tail = with_loss(loss_ref[...])
    for k in range(CORES):
        block = (core_ref[0] + k) % CORES
        share_refs[k][0:SHARE, :] = share_s[pl.ds(pl.multiple_of(block * SHARE, SHARE), SHARE), :].astype(bf16)
        share_refs[k][SHARE:, :] = tail


def final(core, dps, dqa, dqb, projected, hidden, loss):
    return pl.pallas_call(
        final_kernel,
        in_specs=[SM] + [VM] * (X_PEERS + 5),
        out_specs=[VM] * (CORES + 1),
        out_shape=[jax.ShapeDtypeStruct((P_ROWS, EMB), f32)]
        + [jax.ShapeDtypeStruct((SHARE + 8, EMB), bf16)] * CORES,
        scratch_shapes=[
            pltpu.VMEM((EMB, Q_ROWS), bf16),
            pltpu.VMEM((P_ROWS, EMB), f32),
            pltpu.VMEM((CORES * SHARE, EMB), f32),
        ],
        compiler_params=pltpu.CompilerParams(vmem_limit_bytes=12 << 20),
        name="final_grad",
    )(core, *dps, dqa, dqb, projected, hidden, loss)


def combine_kernel(*refs):
    *ins, out_ref = refs
    vals = [r[...].astype(f32) for r in ins]
    total = vals[0] + vals[1] if len(vals) == 2 else (vals[0] + vals[2]) + (vals[1] + vals[3])
    out_ref[0:SHARE, :] = total[0:SHARE].astype(bf16)
    out_ref[SHARE:, :] = with_loss(total[SHARE : SHARE + 1] + total[SHARE + 1 : SHARE + 2])


def combine(parts):
    return pl.pallas_call(
        combine_kernel,
        in_specs=[VM] * len(parts),
        out_specs=VM,
        out_shape=jax.ShapeDtypeStruct((SHARE + 8, EMB), bf16),
        compiler_params=pltpu.CompilerParams(vmem_limit_bytes=4 << 20),
        name="combine",
    )(*parts)


def assemble_kernel(core_ref, *refs):
    *ins, out_ref = refs
    for k in range(CORES):
        block = (core_ref[0] + k) % CORES
        out_ref[pl.ds(pl.multiple_of(block * SHARE, SHARE), SHARE), :] = ins[k][0:SHARE, :].astype(f32)


def assemble(core, parts):
    return pl.pallas_call(
        assemble_kernel,
        in_specs=[SM] + [VM] * len(parts),
        out_specs=VM,
        out_shape=jax.ShapeDtypeStruct((CORES * SHARE, EMB), f32),
        compiler_params=pltpu.CompilerParams(vmem_limit_bytes=4 << 20),
        name="assemble",
    )(core, *parts)


def x_ring(k):
    return [(j, (j // 4) * 4 + (j % 4 + k) % 4) for j in range(32)]


def z_ring(k):
    return [(j, (j // 16 * 4 + (j // 4 % 4 + k) % 4) * 4 + j % 4) for j in range(32)]


def y_swap():
    return [(j, (j + 16) % 32) for j in range(32)]


def y_ring(k):
    def to(j):
        rep, dp = j // 32, j % 32
        y = (rep // 2 * 2 + dp // 16 + k) % 4
        return (y // 2 * 2 + rep % 2) * 32 + y % 2 * 16 + dp % 16

    return [(j, to(j)) for j in range(128)]


def inverse(pairs):
    return [(b, a) for a, b in pairs]


def per_device(
    query_states, passage_states, query_lengths, passage_lengths, passage_ids, positives,
    up_weight, up_bias, down_weight, down_bias, norm_gain, norm_bias, proj_weight,
):
    p_dev, p_len, _ = passage_states.shape
    queries = query_states.shape[0] * lax.axis_size("rep") * lax.axis_size("dp")
    me = lax.axis_index("dp").reshape(1)
    hidden, projected, qsend, psend = encode(
        query_states, jnp.swapaxes(passage_states, 0, 1), query_lengths, passage_lengths, passage_ids,
        positives, up_weight, up_bias, down_weight, down_bias, norm_gain, norm_bias, proj_weight,
    )
    other = lax.ppermute(qsend, "dp", y_swap())
    ps = [psend] + [lax.ppermute(psend, "dp", x_ring(k)) for k in range(1, X_PEERS)]
    pair = jnp.stack([qsend, other])
    qs = [pair] + [lax.ppermute(pair, "dp", z_ring(k)) for k in range(1, 4)]
    sc, tot, zpart, e, pt = forward(me, qs, ps)
    za = zpart + sum(lax.ppermute(zpart, "dp", z_ring(k)) for k in range(1, 4))
    zb = lax.ppermute(za, "dp", y_swap())
    dps, dqs, loss = backward(me, qs, pt, sc, tot, za, zb, e)
    dq = dqs[0].astype(f32)
    for k in range(1, 4):
        dq = dq + lax.ppermute(dqs[k], "dp", inverse(z_ring(k))).astype(f32)
    dps = [dps[0]] + [lax.ppermute(dps[k], "dp", inverse(x_ring(k))) for k in range(1, X_PEERS)]
    dqb = lax.ppermute(dq[1].astype(bf16), "dp", y_swap())
    core = (lax.axis_index("rep") % CORES).reshape(1)
    swap = [(0, 1), (1, 0), (2, 3), (3, 2)]
    pgrad, *shares = final(core, dps, dq[0], dqb, projected, hidden, loss)
    passage_grad = jnp.swapaxes(pgrad.reshape(p_len, p_dev, EMB), 0, 1)
    part = combine([shares[0], lax.ppermute(shares[1], "rep", swap)])
    part = combine([part] + [lax.ppermute(part, "dp", x_ring(k)) for k in range(1, X_PEERS)])
    part = combine([part] + [lax.ppermute(part, "dp", z_ring(k)) for k in range(1, 4)])
    part = combine([part] + [lax.ppermute(part, ("rep", "dp"), y_ring(k)) for k in range(1, 4)])
    mean_loss = (part[SHARE, 0].astype(f32) + part[SHARE + 1, 0].astype(f32)) / queries
    proj_grad = assemble(core, [part, lax.ppermute(part, "rep", swap)])
    return (mean_loss, passage_grad, proj_grad)


def solution(mesh):
    rows = P(("rep", "dp"))
    in_specs = (rows,) * 6 + (P(),) * 7
    out_specs = (P(), rows, P())
    return jax.shard_map(
        per_device, mesh=mesh, in_specs=in_specs, out_specs=out_specs, check_vma=False
    )
```

```python
import jax
import jax.numpy as jnp
from jax import lax
from jax.experimental import pallas as pl
from jax.experimental.pallas import tpu as pltpu
from jax.sharding import PartitionSpec as P

temper = 0.05
eps_norm = 1e-06
punct_low = 999
punct_high = 1067

bf16 = jnp.bfloat16
f32 = jnp.float32
i32 = jnp.int32


X_PEERS = 4
YZ_PEERS = 8
P_ROWS = 720
Q_ROWS = 256
EMB = 128
FCHUNK = 512
ROW_TILES = [slice(0, 256), slice(256, 496), slice(496, 736), slice(736, 976)]
SHARE = 384
CORES = 2
MASKED = 2.0
BIAS = -10000.0
SCALE = 1.4426950408889634 / temper

VM = pl.BlockSpec(memory_space=pltpu.VMEM)
SM = pl.BlockSpec(memory_space=pltpu.SMEM)


def mm(a, b):
    return jnp.dot(a, b, preferred_element_type=f32)


def fetch(which, k, w1_ref, w2_ref, w1_s, w2_s, sem):
    c = pl.ds(pl.multiple_of(k * FCHUNK, FCHUNK), FCHUNK)
    if which == 0:
        return pltpu.make_async_copy(w1_ref.at[:, c], w1_s.at[k], sem.at[0, k])
    return pltpu.make_async_copy(w2_ref.at[c, :], w2_s.at[k], sem.at[1, k])


def feed_forward(w1_ref, b1_s, w2_ref, x_s, acc_s, act_s, w1_s, w2_s, sem, finish):
    count = w1_s.shape[0]

    def up(k, slot):
        bias = b1_s[:, pl.ds(pl.multiple_of(k * FCHUNK, FCHUNK), FCHUNK)]
        val = mm(x_s[...], w1_s[k]) + bias
        act_s[slot] = (val * 0.5 * (1.0 + lax.erf(val * 0.7071067811865476))).astype(bf16)

    fetch(0, 0, w1_ref, w2_ref, w1_s, w2_s, sem).wait()
    up(0, 0)

    def step(k, carry):
        @pl.when(k + 2 < count)
        def _():
            fetch(0, k + 2, w1_ref, w2_ref, w1_s, w2_s, sem).start()
            fetch(1, k + 2, w1_ref, w2_ref, w1_s, w2_s, sem).start()

        fetch(1, k, w1_ref, w2_ref, w1_s, w2_s, sem).wait()
        fetch(0, k + 1, w1_ref, w2_ref, w1_s, w2_s, sem).wait()
        up(k + 1, (k + 1) % 2)
        acc_s[...] += mm(act_s[k % 2], w2_s[k])
        return carry

    lax.fori_loop(0, count - 1, step, 0)
    fetch(1, count - 1, w1_ref, w2_ref, w1_s, w2_s, sem).wait()
    for m, r in enumerate(ROW_TILES):
        finish(m, r, acc_s[r, :] + mm(act_s[(count - 1) % 2, r, :], w2_s[count - 1]))


def finish_rows(r, res, gain, nbias, proj_ref, hidden_ref, projected_ref):
    width = res.shape[1]
    mean = jnp.sum(res, -1, keepdims=True) * (1.0 / width)
    cen = res - mean
    var = jnp.sum(cen * cen, -1, keepdims=True) * (1.0 / width)
    hid = (cen * lax.rsqrt(var + eps_norm) * gain + nbias).astype(bf16)
    hidden_ref[r, :] = hid
    pr = mm(hid, proj_ref[...])
    projected_ref[r, :] = pr
    return pr * lax.rsqrt(jnp.sum(pr * pr, -1, keepdims=True) + eps_norm)


def encode_kernel(
    qlen_any, pos_any, plen_any, ids_any, xq_any, xp_any, w1_ref, b1_any, w2_ref, b2_any,
    gain_any, nbias_any, proj_any, hidden_any, projected_any, qsend_any, psend_any,
    x_s, acc_s, act_s, w1_s, w2_s, sem, keep_s, ids_s, small_sem,
    qlen_ref, pos_ref, plen_ref, ids_ref, xq_ref, xp_ref, b1_ref, b2_ref, gain_ref, nbias_ref, proj_ref,
    hidden_ref, projected_ref, qsend_ref, psend_ref, out_sem,
):
    sources = (xp_any, xq_any, b2_any, ids_any, plen_any, b1_any, gain_any, nbias_any, proj_any, qlen_any, pos_any)
    targets = (xp_ref, xq_ref, b2_ref, ids_ref, plen_ref, b1_ref, gain_ref, nbias_ref, proj_ref, qlen_ref, pos_ref)
    copies = [pltpu.make_async_copy(a, b, small_sem.at[i]) for i, (a, b) in enumerate(zip(sources, targets))]
    for copy in copies[:2]:
        copy.start()
    fetch(0, 0, w1_ref, w2_ref, w1_s, w2_s, sem).start()
    for copy in copies[2:]:
        copy.start()
    q_dev, q_len, width = xq_ref.shape
    p_len, p_dev, _ = xp_ref.shape
    for copy in copies:
        copy.wait()
    fetch(1, 0, w1_ref, w2_ref, w1_s, w2_s, sem).start()
    for which in range(2):
        fetch(which, 1, w1_ref, w2_ref, w1_s, w2_s, sem).start()
    b2, gain, nbias = (v[...].reshape(1, width) for v in (b2_ref, gain_ref, nbias_ref))
    x_s[0:Q_ROWS, :] = xq_ref[...].reshape(Q_ROWS, width)
    x_s[Q_ROWS:, :] = xp_ref[...].reshape(P_ROWS, width)
    acc_s[...] = x_s[...].astype(f32) + b2
    ids_s[...] = jnp.zeros_like(ids_s)
    ids_s[0:p_dev, 0:p_len] = ids_ref[...]
    ids_s[p_dev : 2 * p_dev, 0:p_len] = ids_ref[...]
    ids = ids_s[...]
    row = lax.broadcasted_iota(i32, (8, 256), 0) % p_dev
    col = lax.broadcasted_iota(i32, (8, 256), 1)
    lens = jnp.zeros((8, 256), i32)
    for p in range(p_dev):
        lens = jnp.where(row == p, plen_ref[p], lens)
    punct = jnp.logical_and(ids >= punct_low, ids < punct_high)
    keep = jnp.where(jnp.logical_and(col < lens, jnp.logical_not(punct)), 1.0, 0.0)
    ones = jnp.ones((256, EMB), bf16)
    slab = lax.broadcasted_iota(i32, (30, 8, 256), 0) * 2 + lax.broadcasted_iota(i32, (30, 8, 256), 1) // p_dev
    cols = lax.broadcasted_iota(i32, (30, 8, 256), 2)
    for m in range(3):
        pick = jnp.where(slab + m * 60 == cols, jnp.broadcast_to(keep[None], (30, 8, 256)), 0.0)
        keep_s[m * 240 : (m + 1) * 240, :] = mm(pick.reshape(240, 256).astype(bf16), ones)
    row = lax.broadcasted_iota(i32, (16, EMB), 0)
    token = lax.broadcasted_iota(i32, (16, EMB), 1) + EMB * (row % 2)
    owner = token // q_len
    slot = token % q_len
    lens = jnp.zeros((16, EMB), i32)
    posi = jnp.zeros((16, EMB), i32)
    for q in range(q_dev):
        lens = jnp.where(owner == q, qlen_ref[q], lens)
        posi = jnp.where(owner == q, pos_ref[q], posi)
    kept = jnp.where(slot < lens, 1.0, 0.0)
    meta = jnp.where(row < 2, kept, jnp.where(row < 4, posi.astype(f32), 0.0)).astype(bf16)
    qsend_ref[Q_ROWS : Q_ROWS + 16, :] = meta
    outs = []

    def put(src, dst):
        outs.append(pltpu.make_async_copy(src, dst, out_sem.at[len(outs)]))
        outs[-1].start()

    def finish(m, r, res):
        normed = finish_rows(r, res, gain, nbias, proj_ref, hidden_ref, projected_ref)
        if m == 0:
            qsend_ref[r, :] = normed.astype(bf16)
            put(qsend_ref, qsend_any)
        else:
            s = slice(r.start - Q_ROWS, r.stop - Q_ROWS)
            psend_ref[s, :] = jnp.where(keep_s[s, :] > 0.5, normed, MASKED).astype(bf16)
            put(psend_ref.at[s, :], psend_any.at[s, :])
        put(hidden_ref.at[r, :], hidden_any.at[r, :])
        put(projected_ref.at[r, :], projected_any.at[r, :])

    feed_forward(w1_ref, b1_ref, w2_ref, x_s, acc_s, act_s, w1_s, w2_s, sem, finish)
    for copy in outs:
        copy.wait()


def encode(xq, xp, qlen, plen, ids, pos, w1, b1, w2, b2, gain, nbias, proj):
    width, ff = w1.shape
    count = ff // FCHUNK
    rows = Q_ROWS + P_ROWS
    far = pl.BlockSpec(memory_space=pltpu.HBM)
    return pl.pallas_call(
        encode_kernel,
        in_specs=[far] * 13,
        out_specs=[far] * 4,
        out_shape=[
            jax.ShapeDtypeStruct((rows, width), bf16),
            jax.ShapeDtypeStruct((rows, EMB), f32),
            jax.ShapeDtypeStruct((Q_ROWS + 16, EMB), bf16),
            jax.ShapeDtypeStruct((P_ROWS, EMB), bf16),
        ],
        scratch_shapes=[
            pltpu.VMEM((rows, width), bf16),
            pltpu.VMEM((rows, width), f32),
            pltpu.VMEM((2, rows, FCHUNK), bf16),
            pltpu.VMEM((count, width, FCHUNK), bf16),
            pltpu.VMEM((count, FCHUNK, width), bf16),
            pltpu.SemaphoreType.DMA((2, count)),
            pltpu.VMEM((P_ROWS, EMB), f32),
            pltpu.VMEM((8, 256), i32),
            pltpu.SemaphoreType.DMA((11,)),
            pltpu.SMEM(qlen.shape, i32),
            pltpu.SMEM(pos.shape, i32),
            pltpu.SMEM(plen.shape, i32),
            pltpu.VMEM(ids.shape, i32),
            pltpu.VMEM(xq.shape, bf16),
            pltpu.VMEM(xp.shape, bf16),
            pltpu.VMEM((1, ff), f32),
            pltpu.VMEM((width,), f32),
            pltpu.VMEM((width,), f32),
            pltpu.VMEM((width,), f32),
            pltpu.VMEM(proj.shape, bf16),
            pltpu.VMEM((rows, width), bf16),
            pltpu.VMEM((rows, EMB), f32),
            pltpu.VMEM((Q_ROWS + 16, EMB), bf16),
            pltpu.VMEM((P_ROWS, EMB), bf16),
            pltpu.SemaphoreType.DMA((3 * len(ROW_TILES),)),
        ],
        cost_estimate=pl.CostEstimate(flops=4 * rows * width * ff, bytes_accessed=4 * width * ff, transcendentals=rows * ff),
        name="encode",
    )(qlen, pos, plen, ids, xq, xp, w1, b1[None], w2, b2, gain, nbias, proj)


def load_pairs(q_refs, p_refs, qt_s, pa_s, keep_s):
    for k in range(YZ_PEERS):
        q_ref = q_refs[k // 2]
        qt_s[0:EMB, k * 256 : (k + 1) * 256] = q_ref[k % 2, 0:Q_ROWS, :].T
        for h in range(2):
            keep_s[:, k * 256 + h * 128 : k * 256 + (h + 1) * 128] = q_ref[k % 2, 256 + h : 257 + h, :].astype(f32)
    cols = qt_s.shape[1]
    first = lax.broadcasted_iota(i32, (EMB, cols), 0) == 0
    qt_s[EMB : 2 * EMB, :] = jnp.where(first, 1.0, 0.0).astype(bf16)
    for k, p_ref in enumerate(p_refs):
        r = slice(k * P_ROWS, (k + 1) * P_ROWS)
        val = p_ref[...]
        pa_s[r, 0:EMB] = val
        pa_s[r, EMB : 2 * EMB] = jnp.where(val > bf16(1.5), bf16(BIAS), bf16(0.0))


def origin(me, block):
    yz = me // X_PEERS
    y = (yz // 4 + block % 2) % 2
    return y * 4 + (yz % 4 + 4 - block // 2) % 4


def forward_kernel(me_ref, *refs):
    q_refs, p_refs = refs[:4], refs[4 : 4 + X_PEERS]
    sc_ref, tot_ref, zpart_ref, e_ref, pt_ref, qt_s, pa_s, keep_s, sum_s = refs[4 + X_PEERS :]
    load_pairs(q_refs, p_refs, qt_s, pa_s, keep_s)
    for i in range(0, pa_s.shape[0], 128):
        n = min(128, pa_s.shape[0] - i)
        pt_ref[:, i : i + n] = pa_s[i : i + n, 0:EMB].T
    cols = qt_s.shape[1]

    def group(g, carry):
        for j in range(cols // 256):
            c = slice(j * 256, (j + 1) * 256)
            total = jnp.zeros((8, 256), f32)
            for m in range(3):
                r = pl.ds(pl.multiple_of(g * P_ROWS + m * 240, 16), 240)
                e = jnp.exp2(mm(pa_s[r, :], qt_s[:, c]) * SCALE)
                e_ref[r, c] = e.astype(bf16)
                total = total + jnp.sum(e.reshape(30, 8, 256), axis=0)
            sum_s[pl.ds(pl.multiple_of(g * 8, 8), 8), c] = total
        return carry

    lax.fori_loop(0, X_PEERS, group, 0)
    for g in range(X_PEERS):
        tot_ref[4 * g : 4 * g + 4, :] = sum_s[8 * g : 8 * g + 4, :] + sum_s[8 * g + 4 : 8 * g + 8, :]
    a = lax.broadcasted_iota(i32, (128, 128), 0) // 32
    b = lax.broadcasted_iota(i32, (128, 128), 1) // 32
    same = jnp.where(a == b, 1.0, 0.0)
    for t in range(cols // 128):
        c = slice(t * 128, (t + 1) * 128)
        soft = jnp.log(tot_ref[:, c]) * temper * keep_s[:, c]
        sc = jnp.dot(soft, same, preferred_element_type=f32, precision=lax.Precision.HIGHEST)
        sc_ref[:, c] = sc
        z = jnp.sum(jnp.exp(sc), axis=0, keepdims=True)
        zpart_ref[pl.ds(origin(me_ref[0], t // 2) * 2 + t % 2, 1), :] = z


def forward(me, qs, ps):
    cols = YZ_PEERS * Q_ROWS
    return pl.pallas_call(
        forward_kernel,
        in_specs=[SM] + [VM] * (4 + X_PEERS),
        out_specs=[VM] * 5,
        out_shape=[
            jax.ShapeDtypeStruct((16, cols), f32),
            jax.ShapeDtypeStruct((16, cols), f32),
            jax.ShapeDtypeStruct((16, 128), f32),
            jax.ShapeDtypeStruct((X_PEERS * P_ROWS, cols), bf16),
            jax.ShapeDtypeStruct((EMB, X_PEERS * P_ROWS), bf16),
        ],
        scratch_shapes=[
            pltpu.VMEM((256, cols), bf16),
            pltpu.VMEM((X_PEERS * P_ROWS, 256), bf16),
            pltpu.VMEM((1, cols), f32),
            pltpu.VMEM((8 * X_PEERS, cols), f32),
        ],
        compiler_params=pltpu.CompilerParams(vmem_limit_bytes=16 << 20),
        name="pair_forward",
    )(me, *qs, *ps)


def backward_kernel(me_ref, *refs):
    q_refs, refs = refs[:4], refs[4:]
    pt_ref, sc_ref, tot_ref, za_ref, zb_ref, e_ref = refs[:6]
    dp_refs, dq_refs, refs = refs[6 : 6 + X_PEERS], refs[6 + X_PEERS : 10 + X_PEERS], refs[10 + X_PEERS :]
    loss_ref, q_s, fac_s, g_s, dp_s = refs
    p_all, cols = g_s.shape
    for k in range(YZ_PEERS):
        q_s[k * 256 : (k + 1) * 256, :] = q_refs[k // 2][k % 2, 0:Q_ROWS, :]
    me = me_ref[0]
    x = me % X_PEERS
    row = lax.broadcasted_iota(i32, (16, 128), 0)
    number = row % 4 + (me // X_PEERS) * 16
    for k in range(X_PEERS):
        number = jnp.where(row // 4 == k, number + ((x + X_PEERS - k) % X_PEERS) * 4, number)
    number = number.astype(f32)
    lane = lax.broadcasted_iota(i32, (1, 128), 1)
    head = jnp.where(lane % 32 == 0, 1.0, 0.0)
    loss = jnp.zeros((1, 128), f32)
    for t in range(cols // 128):
        c = slice(t * 128, (t + 1) * 128)
        at = pl.ds(origin(me, t // 2) * 2 + t % 2, 1)
        z = za_ref[at, :] + zb_ref[at, :]
        sc = sc_ref[:, c]
        q_ref, a = q_refs[t // 4], t // 2 % 2
        keep = q_ref[a, 256 + t % 2 : 257 + t % 2, :].astype(f32)
        pos = q_ref[a, 258 + t % 2 : 259 + t % 2, :].astype(f32)
        hit = jnp.where(number == pos, 1.0, 0.0)
        fac = (jnp.exp(sc) / z - hit) * (keep / tot_ref[:, c])
        for g in range(X_PEERS):
            fac_s[8 * g : 8 * g + 4, c] = fac[4 * g : 4 * g + 4, :]
            fac_s[8 * g + 4 : 8 * g + 8, c] = fac[4 * g : 4 * g + 4, :]
        loss = loss + (jnp.log(z) * (1.0 / YZ_PEERS) - jnp.sum(hit * sc, axis=0, keepdims=True)) * head
    loss_ref[...] = jnp.broadcast_to(jnp.sum(loss, axis=1, keepdims=True), loss_ref.shape)

    def group(g, carry):
        for m in range(3):
            r = pl.ds(pl.multiple_of(g * P_ROWS + m * 240, 16), 240)
            for j in range(cols // 256):
                c = slice(j * 256, (j + 1) * 256)
                fac = fac_s[pl.ds(pl.multiple_of(g * 8, 8), 8), c]
                grad = e_ref[r, c].astype(f32).reshape(30, 8, 256) * fac[None]
                g_s[r, c] = grad.reshape(240, 256).astype(bf16)
            dp_s[r, :] = mm(g_s[r, :], q_s[...])
        return carry

    lax.fori_loop(0, X_PEERS, group, 0)

    for k in range(4):
        dq = mm(pt_ref[...], g_s[:, k * 512 : (k + 1) * 512]).astype(bf16)
        for h in range(2):
            dq_refs[k][h] = dq[:, h * 256 : (h + 1) * 256]
    for k in range(X_PEERS):
        dp_refs[k][...] = dp_s[k * P_ROWS : (k + 1) * P_ROWS, :].astype(dp_refs[k].dtype)


def backward(me, qs, pt, sc, tot, za, zb, e):
    p_all, cols = e.shape
    out = pl.pallas_call(
        backward_kernel,
        in_specs=[SM] + [VM] * 10,
        out_specs=[VM] * (X_PEERS + 5),
        out_shape=[jax.ShapeDtypeStruct((P_ROWS, EMB), f32 if k == 0 else bf16) for k in range(X_PEERS)]
        + [jax.ShapeDtypeStruct((2, EMB, Q_ROWS), bf16)] * 4
        + [jax.ShapeDtypeStruct((1, 128), f32)],
        scratch_shapes=[
            pltpu.VMEM((cols, EMB), bf16),
            pltpu.VMEM((8 * X_PEERS, cols), f32),
            pltpu.VMEM((p_all, cols), bf16),
            pltpu.VMEM((p_all, EMB), f32),
        ],
        compiler_params=pltpu.CompilerParams(vmem_limit_bytes=24 << 20),
        name="pair_backward",
    )(me, *qs, pt, sc, tot, za, zb, e)
    return out[:X_PEERS], out[X_PEERS : X_PEERS + 4], out[-1]


def with_loss(loss):
    row = lax.broadcasted_iota(i32, (8, EMB), 0)
    high = loss.astype(bf16).astype(f32)
    return jnp.where(row == 0, high, jnp.where(row == 1, loss - high, 0.0)).astype(bf16)


def final_kernel(core_ref, *refs):
    dp_refs, refs = refs[:X_PEERS], refs[X_PEERS:]
    dqa_ref, dqb_ref, projected_ref, hidden_ref, loss_ref, pgrad_ref = refs[:6]
    share_refs = refs[6 : 6 + CORES]
    bt_s, bp_s, share_s = refs[6 + CORES :]
    pr = projected_ref[0:Q_ROWS, :]
    inv = lax.rsqrt(jnp.sum(pr * pr, -1, keepdims=True) + eps_norm)
    nt = (pr * inv).T
    it = jnp.broadcast_to(inv, pr.shape).T
    grad = dqa_ref[...] + dqb_ref[...].astype(f32)
    dot = jnp.sum(nt * grad, axis=0, keepdims=True)
    bt_s[...] = (it * (grad - nt * dot)).astype(bf16)
    for m in range(3):
        r = slice(m * 240, (m + 1) * 240)
        grad = dp_refs[0][r, :].astype(f32)
        for k in range(1, X_PEERS):
            grad = grad + dp_refs[k][r, :].astype(f32)
        pgrad_ref[r, :] = grad
        pr = projected_ref[Q_ROWS + m * 240 : Q_ROWS + (m + 1) * 240, :]
        inv = lax.rsqrt(jnp.sum(pr * pr, -1, keepdims=True) + eps_norm)
        nm = pr * inv
        bp_s[r, :] = inv * (grad - nm * jnp.sum(nm * grad, -1, keepdims=True))
    bpt = bp_s[...].T.astype(bf16)
    for k in range(6):
        c = slice(k * 128, (k + 1) * 128)
        pg = mm(bt_s[...], hidden_ref[0:Q_ROWS, c]) + mm(bpt, hidden_ref[Q_ROWS:, c])
        share_s[c, :] = pg.T
    tail = with_loss(loss_ref[...])
    for k in range(CORES):
        block = (core_ref[0] + k) % CORES
        share_refs[k][0:SHARE, :] = share_s[pl.ds(pl.multiple_of(block * SHARE, SHARE), SHARE), :].astype(bf16)
        share_refs[k][SHARE:, :] = tail


def final(core, dps, dqa, dqb, projected, hidden, loss):
    return pl.pallas_call(
        final_kernel,
        in_specs=[SM] + [VM] * (X_PEERS + 5),
        out_specs=[VM] * (CORES + 1),
        out_shape=[jax.ShapeDtypeStruct((P_ROWS, EMB), f32)]
        + [jax.ShapeDtypeStruct((SHARE + 8, EMB), bf16)] * CORES,
        scratch_shapes=[
            pltpu.VMEM((EMB, Q_ROWS), bf16),
            pltpu.VMEM((P_ROWS, EMB), f32),
            pltpu.VMEM((CORES * SHARE, EMB), f32),
        ],
        compiler_params=pltpu.CompilerParams(vmem_limit_bytes=12 << 20),
        name="final_grad",
    )(core, *dps, dqa, dqb, projected, hidden, loss)


def combine_kernel(*refs):
    *ins, out_ref = refs
    vals = [r[...].astype(f32) for r in ins]
    total = vals[0] + vals[1] if len(vals) == 2 else (vals[0] + vals[2]) + (vals[1] + vals[3])
    out_ref[0:SHARE, :] = total[0:SHARE].astype(bf16)
    out_ref[SHARE:, :] = with_loss(total[SHARE : SHARE + 1] + total[SHARE + 1 : SHARE + 2])


def combine(parts):
    return pl.pallas_call(
        combine_kernel,
        in_specs=[VM] * len(parts),
        out_specs=VM,
        out_shape=jax.ShapeDtypeStruct((SHARE + 8, EMB), bf16),
        compiler_params=pltpu.CompilerParams(vmem_limit_bytes=4 << 20),
        name="combine",
    )(*parts)


def assemble_kernel(core_ref, *refs):
    *ins, out_ref = refs
    for k in range(CORES):
        block = (core_ref[0] + k) % CORES
        out_ref[pl.ds(pl.multiple_of(block * SHARE, SHARE), SHARE), :] = ins[k][0:SHARE, :].astype(f32)


def assemble(core, parts):
    return pl.pallas_call(
        assemble_kernel,
        in_specs=[SM] + [VM] * len(parts),
        out_specs=VM,
        out_shape=jax.ShapeDtypeStruct((CORES * SHARE, EMB), f32),
        compiler_params=pltpu.CompilerParams(vmem_limit_bytes=4 << 20),
        name="assemble",
    )(core, *parts)


def x_ring(k):
    return [(j, (j // 4) * 4 + (j % 4 + k) % 4) for j in range(32)]


def z_ring(k):
    return [(j, (j // 16 * 4 + (j // 4 % 4 + k) % 4) * 4 + j % 4) for j in range(32)]


def y_swap():
    return [(j, (j + 16) % 32) for j in range(32)]


def y_ring(k):
    def to(j):
        rep, dp = j // 32, j % 32
        y = (rep // 2 * 2 + dp // 16 + k) % 4
        return (y // 2 * 2 + rep % 2) * 32 + y % 2 * 16 + dp % 16

    return [(j, to(j)) for j in range(128)]


def inverse(pairs):
    return [(b, a) for a, b in pairs]


def per_device(
    query_states, passage_states, query_lengths, passage_lengths, passage_ids, positives,
    up_weight, up_bias, down_weight, down_bias, norm_gain, norm_bias, proj_weight,
):
    p_dev, p_len, _ = passage_states.shape
    queries = query_states.shape[0] * lax.axis_size("rep") * lax.axis_size("dp")
    me = lax.axis_index("dp").reshape(1)
    hidden, projected, qsend, psend = encode(
        query_states, jnp.swapaxes(passage_states, 0, 1), query_lengths, passage_lengths, passage_ids,
        positives, up_weight, up_bias, down_weight, down_bias, norm_gain, norm_bias, proj_weight,
    )
    other = lax.ppermute(qsend, "dp", y_swap())
    ps = [psend] + [lax.ppermute(psend, "dp", x_ring(k)) for k in range(1, X_PEERS)]
    pair = jnp.stack([qsend, other])
    qs = [pair] + [lax.ppermute(pair, "dp", z_ring(k)) for k in range(1, 4)]
    sc, tot, zpart, e, pt = forward(me, qs, ps)
    za = zpart + sum(lax.ppermute(zpart, "dp", z_ring(k)) for k in range(1, 4))
    zb = lax.ppermute(za, "dp", y_swap())
    dps, dqs, loss = backward(me, qs, pt, sc, tot, za, zb, e)
    dq = dqs[0].astype(f32)
    for k in range(1, 4):
        dq = dq + lax.ppermute(dqs[k], "dp", inverse(z_ring(k))).astype(f32)
    dps = [dps[0]] + [lax.ppermute(dps[k], "dp", inverse(x_ring(k))) for k in range(1, X_PEERS)]
    dqb = lax.ppermute(dq[1].astype(bf16), "dp", y_swap())
    core = (lax.axis_index("rep") % CORES).reshape(1)
    swap = [(0, 1), (1, 0), (2, 3), (3, 2)]
    pgrad, *shares = final(core, dps, dq[0], dqb, projected, hidden, loss)
    passage_grad = jnp.swapaxes(pgrad.reshape(p_len, p_dev, EMB), 0, 1)
    part = combine([shares[0], lax.ppermute(shares[1], "rep", swap)])
    part = combine([part] + [lax.ppermute(part, "dp", x_ring(k)) for k in range(1, X_PEERS)])
    part = combine([part] + [lax.ppermute(part, "dp", z_ring(k)) for k in range(1, 4)])
    part = combine([part] + [lax.ppermute(part, ("rep", "dp"), y_ring(k)) for k in range(1, 4)])
    mean_loss = (part[SHARE, 0].astype(f32) + part[SHARE + 1, 0].astype(f32)) / queries
    proj_grad = assemble(core, [part, lax.ppermute(part, "rep", swap)])
    return (mean_loss, passage_grad, proj_grad)


def solution(mesh):
    rows = P(("rep", "dp"))
    in_specs = (rows,) * 6 + (P(),) * 7
    out_specs = (P(), rows, P())
    return jax.shard_map(
        per_device, mesh=mesh, in_specs=in_specs, out_specs=out_specs, check_vma=False
    )
```
